32 devices in a mesh: spin: 2 (over core), band: 8 (over z, x), grid: 2 (over y).
Axes of the slice: x: 2, y: 2, z: 4, core: 2. Of those that a mesh axis runs over, the one named last changes fastest.
Arguments:
- orbitals: bfloat16 [2, 64, 128, 128, 128], P('spin', 'band', 'grid'), may hold values from -0.14941406 to 0.14941406
- partial_bands: int32 [2, 2], P('spin'), may hold values from 0 to 63
- core_density: float32 [128, 128, 128], P('grid'), may hold values from 0.002 to 0.2
Outputs:
- potential: float32 [2, 128, 128, 128], P('spin', 'grid', 'band')
The draws below stay inside these ranges and needn't reach their ends.
Inputs may be any that keep to these rules, and one draw needn't show every extreme that they name: `partial_bands`: row s holds, for spin s, the first half-occupied band and the count of half-occupied bands; bands past 64 - 1 do not exist.
All inputs are finite; a program needn't handle non-finite values.
Results may differ from the reference program's by a relative error of at most 0.0003.
Values sent between devices are 32-bit elements; how exact they have to be, the bound alone decides.
A program may use at most 128 MiB of HBM per device.

```python
import math
import jax
import jax.numpy as jnp
from jax import lax

NX = 128
NY = 128
NZ = 128
SPINS = 2
BANDS = 64


def set_ends(drawn, own_key, smallest, high):
    extent = drawn.shape
    spot = [jax.random.randint(jax.random.fold_in(own_key, axis), (), 0, extent[axis]) for axis in range(len(extent))]
    drawn = drawn.at[tuple(spot)].set(smallest)
    longest = extent.index(max(extent))
    spot[longest] = (spot[longest] + 1) % extent[longest]
    return drawn.at[tuple(spot)].set(high)


def shard_levels(own_key, shape, pieces, least, top_value):
    def one(axis_at, parts):
        steps = jax.random.uniform(jax.random.fold_in(jax.random.fold_in(own_key, 6), axis_at), (parts,), jnp.float32, least / len(pieces), top_value / len(pieces))
        return jnp.repeat(jnp.exp(steps), shape[axis_at] // parts).reshape((-1,) + (1,) * (len(shape) - axis_at - 1))

    factor_of = one(*pieces[0])
    for cut in pieces[1:]:
        factor_of = factor_of * one(*cut)
    return factor_of


def noise(key, shape, scale, reach, cuts=(), kind=jnp.bfloat16):
    drawn = scale * jax.random.normal(key, shape, jnp.float32)
    if cuts:
        drawn = drawn * shard_levels(key, shape, cuts, -0.22, 0.18)
    return jnp.clip(drawn, -reach, reach).astype(kind)


def setup_inputs(seed: int = 0) -> dict:
    arg_keys = jax.random.split(jax.random.key(seed), 4)
    return {
        "orbitals": noise(arg_keys[0], (SPINS, BANDS, NX, NY, NZ), 0.025, 0.14941406, ((0, 2), (1, 8), (2, 2))),
        "partial_bands": set_ends(jax.random.randint(arg_keys[1], (SPINS, 2), 0, BANDS), jax.random.fold_in(arg_keys[1], 1), 0, BANDS - 1).astype(jnp.int32),
        "core_density": jnp.clip(jnp.exp(math.log(0.2) - 4.6051702 * jax.random.uniform(arg_keys[2], (NX, NY, NZ), jnp.float32) ** shard_levels(arg_keys[2], (NX, NY, NZ), ((0, 2),), -0.2, 0.2)), 0.002, 0.2),
    }


KAPPA = 0.804
MU_X = 0.2195149727645171
BETA = 0.06672455060314922
GAMMA = (1.0 - math.log(2.0)) / math.pi ** 2
FZ_NORM = 2.0 ** (4.0 / 3.0) - 2.0
FPP_ZERO = 1.709921

def pw_fit(radius, amp, alpha, beta_one, beta_two, beta_three, beta_four):
    root = jnp.sqrt(radius)
    denom = 2.0 * amp * (beta_one * root + beta_two * radius + beta_three * radius * root + beta_four * radius * radius)
    return -2.0 * amp * (1.0 + alpha * radius) * jnp.log(1.0 + 1.0 / denom)

def exchange_part(double, sigma_four):
    kfermi = (3.0 * math.pi ** 2 * double) ** (1.0 / 3.0)
    scaled = sigma_four / (4.0 * kfermi * kfermi * double * double)
    enhance = 1.0 + KAPPA - KAPPA / (1.0 + MU_X * scaled / KAPPA)
    return -0.75 / math.pi * kfermi * double * enhance

def xc_energy(n_up, n_down, s_uu, s_ud, s_dd):
    exch = 0.5 * (exchange_part(2.0 * n_up, 4.0 * s_uu) + exchange_part(2.0 * n_down, 4.0 * s_dd))
    total = n_up + n_down
    zeta = (n_up - n_down) / total
    radius = (3.0 / (4.0 * math.pi * total)) ** (1.0 / 3.0)
    ec_para = pw_fit(radius, 0.031091, 0.2137, 7.5957, 3.5876, 1.6382, 0.49294)
    ec_ferro = pw_fit(radius, 0.015545, 0.20548, 14.1189, 6.1977, 3.3662, 0.62517)
    neg_stiff = pw_fit(radius, 0.016887, 0.11125, 10.357, 3.6231, 0.88026, 0.49671)
    plus_z = 1.0 + zeta
    minus_z = 1.0 - zeta
    fzeta = (plus_z ** (4.0 / 3.0) + minus_z ** (4.0 / 3.0) - 2.0) / FZ_NORM
    zeta_four = zeta ** 4
    ec_lda = ec_para - neg_stiff * fzeta / FPP_ZERO * (1.0 - zeta_four) + (ec_ferro - ec_para) * fzeta * zeta_four
    phi = 0.5 * (plus_z ** (2.0 / 3.0) + minus_z ** (2.0 / 3.0))
    phi_cube = phi * phi * phi
    kfermi = (3.0 * math.pi ** 2 * total) ** (1.0 / 3.0)
    screen_sq = 4.0 * kfermi / math.pi
    sigma = s_uu + 2.0 * s_ud + s_dd
    tsq = sigma / (4.0 * phi * phi * screen_sq * total * total)
    amp = BETA / GAMMA / (jnp.exp(-ec_lda / (GAMMA * phi_cube)) - 1.0)
    atsq = amp * tsq
    gradient_term = GAMMA * phi_cube * jnp.log(1.0 + BETA / GAMMA * tsq * (1.0 + atsq) / (1.0 + atsq + atsq * atsq))
    return exch + total * (ec_lda + gradient_term)

def spectral(field, axis):
    length = field.shape[axis]
    index = jnp.arange(length, dtype=jnp.int32)
    mode = jnp.where(index < length // 2, index, index - length)
    mode = jnp.where(index == length // 2, 0, mode)
    wave = 2.0 * math.pi / length * mode.astype(jnp.float32)
    shape = [1, 1, 1]
    shape[axis] = length
    spec = jnp.fft.fft(field, axis=axis)
    return jnp.real(jnp.fft.ifft(spec * (1j * wave.reshape(shape)), axis=axis)).astype(jnp.float32)

def reference(orbitals, partial_bands, core_density):
    band_ids = jnp.arange(BANDS, dtype=jnp.int32)

    def spin_density(spin_id):
        first = partial_bands[spin_id, 0]
        span = partial_bands[spin_id, 1]
        weights = jnp.where((band_ids >= first) & (band_ids < first + span), 0.5, 1.0).astype(jnp.float32)

        def accumulate(total, item):
            weight, orbital = item
            values = orbital.astype(jnp.float32)
            return (total + weight * values * values, None)
        start = jnp.zeros((NX, NY, NZ), jnp.float32)
        total, unused = lax.scan(accumulate, start, (weights, orbitals[spin_id]))
        return total + 0.5 * core_density
    dens_up = spin_density(0)
    dens_down = spin_density(1)
    grad_up = [spectral(dens_up, axis) for axis in range(3)]
    grad_down = [spectral(dens_down, axis) for axis in range(3)]
    s_uu = grad_up[0] * grad_up[0] + grad_up[1] * grad_up[1] + grad_up[2] * grad_up[2]
    s_ud = grad_up[0] * grad_down[0] + grad_up[1] * grad_down[1] + grad_up[2] * grad_down[2]
    s_dd = grad_down[0] * grad_down[0] + grad_down[1] * grad_down[1] + grad_down[2] * grad_down[2]
    energy, pull = jax.vjp(xc_energy, dens_up, dens_down, s_uu, s_ud, s_dd)
    derivs = pull(jnp.ones_like(energy))
    div_up = jnp.zeros_like(dens_up)
    div_down = jnp.zeros_like(dens_up)
    for axis in range(3):
        flux_up = 2.0 * derivs[2] * grad_up[axis] + derivs[3] * grad_down[axis]
        flux_down = 2.0 * derivs[4] * grad_down[axis] + derivs[3] * grad_up[axis]
        div_up = div_up + spectral(flux_up, axis)
        div_down = div_down + spectral(flux_down, axis)
    return jnp.stack([derivs[0] - div_up, derivs[1] - div_down])
```

```python
import functools
import math

import jax
import jax.numpy as jnp
import numpy as np
from jax import lax
from jax.experimental import pallas as pl
from jax.experimental.pallas import tpu as pltpu
from jax.sharding import PartitionSpec as P

KAPPA = 0.804
MU_X = 0.2195149727645171
BETA = 0.06672455060314922
GAMMA = (1.0 - math.log(2.0)) / math.pi**2
FZ_NORM = 2.0 ** (4.0 / 3.0) - 2.0
FPP_ZERO = 1.709921
EXACT = lax.Precision.HIGHEST
MESH = pl.DeviceIdType.MESH
CHUNK = 4
FAST = 2


def cube_root(value):
    return jnp.exp(jnp.log(value) * (1.0 / 3.0))


def pw_fit(radius, root, amp, alpha, beta_one, beta_two, beta_three, beta_four):
    denom = (2.0 * amp) * (
        root * (beta_one + root * (beta_two + root * (beta_three + root * beta_four)))
    )
    return -2.0 * amp * (1.0 + alpha * radius) * jnp.log(1.0 + 1.0 / denom)


def exchange_part(double, sigma_four):
    kfermi = (3.0 * math.pi**2) ** (1.0 / 3.0) * cube_root(double)
    product = kfermi * double
    scaled = sigma_four / (4.0 * product * product)
    enhance = 1.0 + KAPPA - KAPPA / (1.0 + MU_X * scaled / KAPPA)
    return -0.75 / math.pi * product * enhance


def xc_energy(n_up, n_down, s_uu, s_ud, s_dd):
    exch = 0.5 * (exchange_part(2.0 * n_up, 4.0 * s_uu) + exchange_part(2.0 * n_down, 4.0 * s_dd))
    total = n_up + n_down
    zeta = (n_up - n_down) / total
    third = cube_root(total)
    radius = (3.0 / (4.0 * math.pi)) ** (1.0 / 3.0) / third
    root = jnp.sqrt(radius)
    ec_para = pw_fit(radius, root, 0.031091, 0.2137, 7.5957, 3.5876, 1.6382, 0.49294)
    ec_ferro = pw_fit(radius, root, 0.015545, 0.20548, 14.1189, 6.1977, 3.3662, 0.62517)
    neg_stiff = pw_fit(radius, root, 0.016887, 0.11125, 10.357, 3.6231, 0.88026, 0.49671)
    plus_z = 1.0 + zeta
    minus_z = 1.0 - zeta
    plus_third = cube_root(plus_z)
    minus_third = cube_root(minus_z)
    fzeta = (plus_z * plus_third + minus_z * minus_third - 2.0) * (1.0 / FZ_NORM)
    zeta_sq = zeta * zeta
    zeta_four = zeta_sq * zeta_sq
    ec_lda = (
        ec_para
        - neg_stiff * fzeta * (1.0 / FPP_ZERO) * (1.0 - zeta_four)
        + (ec_ferro - ec_para) * fzeta * zeta_four
    )
    phi = 0.5 * (plus_third * plus_third + minus_third * minus_third)
    phi_cube = phi * phi * phi
    kfermi = (3.0 * math.pi**2) ** (1.0 / 3.0) * third
    screen_sq = kfermi * (4.0 / math.pi)
    sigma = s_uu + 2.0 * s_ud + s_dd
    tsq = sigma / (4.0 * phi * phi * screen_sq * total * total)
    amp = BETA / GAMMA / (jnp.exp(-ec_lda / (GAMMA * phi_cube)) - 1.0)
    atsq = amp * tsq
    gradient_term = (
        GAMMA
        * phi_cube
        * jnp.log(1.0 + BETA / GAMMA * tsq * (1.0 + atsq) / (1.0 + atsq + atsq * atsq))
    )
    return exch + total * (ec_lda + gradient_term)


def spectral_table(length):
    index = np.arange(length)
    angle = 2.0 * np.pi / length * (index[:, None] * index[None, :] % length)
    mode = np.where(index < length // 2, index, index - length)
    mode = np.where(index == length // 2, 0, mode)
    wave = 2.0 * np.pi / length * mode
    sines, cosines = np.sin(angle), np.cos(angle)
    first_term = (sines * wave[None, :]) @ cosines.T
    second_term = (cosines * wave[None, :]) @ sines.T
    return ((second_term - first_term) / length).astype(np.float32)


def greet(partners):
    barrier = pltpu.get_barrier_semaphore()
    for partner in partners:
        pl.semaphore_signal(barrier, inc=1, device_id=partner, device_id_type=MESH)
    pl.semaphore_wait(barrier, len(partners))


def density_kernel(
    bands,
    pairs_ref,
    orb_hbm,
    core_hbm,
    out_ref,
    orb,
    core,
    part,
    x_in,
    z_out,
    z_in,
    orb_sem,
    core_sem,
    x_send,
    x_recv,
    z_send,
    z_recv,
):
    count, rows, y_cells, z_cells = orb.shape
    block = core.shape[1]
    slow = bands // FAST
    chunks = rows // CHUNK
    me = lax.axis_index("band")
    my_slow, my_fast = lax.div(me, FAST), lax.rem(me, FAST)
    partner = {"band": my_slow * FAST + (1 - my_fast)}
    others = [{"band": lax.rem(my_slow + k, slow) * FAST + my_fast} for k in range(1, slow)]

    def orb_copy(c):
        span = pl.ds(c * CHUNK, CHUNK)
        return pltpu.make_async_copy(orb_hbm.at[0, :, span], orb.at[:, span], orb_sem.at[c])

    def core_copy():
        span = pl.ds(pl.multiple_of(me * block, block), block)
        return pltpu.make_async_copy(core_hbm.at[:, span], core, core_sem)

    def x_copy(c):
        span = pl.ds(c * CHUNK, CHUNK)
        return pltpu.make_async_remote_copy(
            src_ref=part.at[1 - my_fast, span],
            dst_ref=x_in.at[span],
            send_sem=x_send.at[c],
            recv_sem=x_recv.at[c],
            device_id=partner,
            device_id_type=MESH,
        )

    def z_copy(c, k):
        span = pl.ds(c * CHUNK, CHUNK)
        return pltpu.make_async_remote_copy(
            src_ref=z_out.at[lax.rem(my_slow + k, slow), span],
            dst_ref=z_in.at[k - 1, span],
            send_sem=z_send.at[k - 1, c],
            recv_sem=z_recv.at[k - 1, c],
            device_id=others[k - 1],
            device_id_type=MESH,
        )

    def each(body):
        lax.fori_loop(0, chunks, lambda c, carry: (body(c), carry)[1], 0)

    each(lambda c: orb_copy(c).start())
    core_copy().start()
    greet([partner] + others)
    first = pairs_ref[0, 0]
    last = first + pairs_ref[0, 1]
    weights = []
    for n in range(count):
        ident = me * count + n
        weights.append(jnp.where((ident >= first) & (ident < last), 0.5, 1.0).astype(jnp.float32))

    def density(c):
        orb_copy(c).wait()
        for r in range(CHUNK):
            row = c * CHUNK + r
            for piece in range(bands):
                total = jnp.zeros((block, z_cells), jnp.float32)
                for n in range(count):
                    values = orb[n, row, piece * block : (piece + 1) * block].astype(jnp.float32)
                    total += weights[n] * (values * values)
                part[piece % FAST, row, piece // FAST] = total
        x_copy(c).start()

    each(density)

    def forward(c):
        x_copy(c).wait_recv()
        span = pl.ds(c * CHUNK, CHUNK)
        for piece in range(slow):
            z_out[piece, span] = part[my_fast, span, piece] + x_in[span, piece]
        for k in range(1, slow):
            z_copy(c, k).start()

    each(forward)
    core_copy().wait()

    def collect(c):
        span = pl.ds(c * CHUNK, CHUNK)
        total = 0.5 * core[span] + z_out[my_slow, span]
        for k in range(1, slow):
            z_copy(c, k).wait_recv()
            total += z_in[k - 1, span]
        out_ref[span] = total

    each(collect)

    def drain(c):
        x_copy(c).wait_send()
        for k in range(1, slow):
            z_copy(c, k).wait_send()

    each(drain)


def own_density(orbitals, partial_bands, core_density):
    bands = lax.axis_size("band")
    _, count, rows, y_cells, z_cells = orbitals.shape
    block = y_cells // bands
    slow = bands // FAST
    chunks = rows // CHUNK
    return pl.pallas_call(
        functools.partial(density_kernel, bands),
        out_shape=jax.ShapeDtypeStruct((rows, block, z_cells), jnp.float32),
        in_specs=[
            pl.BlockSpec(memory_space=pltpu.SMEM),
            pl.BlockSpec(memory_space=pl.ANY),
            pl.BlockSpec(memory_space=pl.ANY),
        ],
        out_specs=pl.BlockSpec(memory_space=pltpu.VMEM),
        scratch_shapes=[
            pltpu.VMEM((count, rows, y_cells, z_cells), jnp.bfloat16),
            pltpu.VMEM((rows, block, z_cells), jnp.float32),
            pltpu.VMEM((FAST, rows, slow, block, z_cells), jnp.float32),
            pltpu.VMEM((rows, slow, block, z_cells), jnp.float32),
            pltpu.VMEM((slow, rows, block, z_cells), jnp.float32),
            pltpu.VMEM((slow - 1, rows, block, z_cells), jnp.float32),
            pltpu.SemaphoreType.DMA((chunks,)),
            pltpu.SemaphoreType.DMA,
            pltpu.SemaphoreType.DMA((chunks,)),
            pltpu.SemaphoreType.DMA((chunks,)),
            pltpu.SemaphoreType.DMA((slow - 1, chunks)),
            pltpu.SemaphoreType.DMA((slow - 1, chunks)),
        ],
        compiler_params=pltpu.CompilerParams(
            collective_id=0, has_side_effects=True, vmem_limit_bytes=48 * 2**20
        ),
        name="band_density",
    )(partial_bands, orbitals, core_density)


def swapped(block, axis, stride):
    count = lax.axis_size(axis)
    route = []
    for low in range(count):
        high = low | 1 << stride
        if high != low and high < count:
            route += [(low, high), (high, low)]
    return lax.ppermute(block, axis, route)


def along_first(stack, table):
    return jnp.einsum("jl,flyz->fjyz", table, stack, precision=EXACT)


def along_second(stack, table):
    return jnp.einsum("jl,fxlz->fxjz", table, stack, precision=EXACT)


def along_third(stack, table):
    return jnp.einsum("fxyl,jl->fxyj", stack, table, precision=EXACT)


def pencil_axes(first, second, third, tables):
    deriv_x = lax.all_to_all(
        along_first(
            lax.all_to_all(first, "grid", split_axis=2, concat_axis=1, tiled=True), tables[0]
        ),
        "grid",
        split_axis=1,
        concat_axis=2,
        tiled=True,
    )
    deriv_y = lax.all_to_all(
        along_second(
            lax.all_to_all(second, "band", split_axis=1, concat_axis=2, tiled=True), tables[1]
        ),
        "band",
        split_axis=2,
        concat_axis=1,
        tiled=True,
    )
    return (deriv_x, deriv_y, along_third(third, tables[2]))


def per_device(orbitals, partial_bands, core_density):
    x_rows, y_cols, z_cells = core_density.shape
    tables = (
        jnp.asarray(spectral_table(x_rows * lax.axis_size("grid"))),
        jnp.asarray(spectral_table(y_cols)),
        jnp.asarray(spectral_table(z_cells)),
    )
    own = own_density(orbitals, partial_bands, core_density)
    single = own[None]
    steep = jnp.concatenate(pencil_axes(single, single, single, tables), axis=0)
    sent = jnp.concatenate([single, steep], axis=0)
    got = swapped(sent, "spin", 0)
    other = got[0]
    other_steep = got[1:]
    is_up = lax.axis_index("spin") == 0
    dens_up = jnp.where(is_up, own, other)
    dens_down = jnp.where(is_up, other, own)
    grad_up = jnp.where(is_up, steep, other_steep)
    grad_down = jnp.where(is_up, other_steep, steep)
    s_uu = jnp.sum(grad_up * grad_up, axis=0)
    s_ud = jnp.sum(grad_up * grad_down, axis=0)
    s_dd = jnp.sum(grad_down * grad_down, axis=0)
    energy, pull = jax.vjp(xc_energy, dens_up, dens_down, s_uu, s_ud, s_dd)
    derivs = pull(jnp.ones_like(energy))
    dn_own = jnp.where(is_up, derivs[0], derivs[1])
    ds_own = jnp.where(is_up, derivs[2], derivs[4])
    flux = 2.0 * ds_own[None] * steep + derivs[3][None] * other_steep
    div_x, div_y, div_z = pencil_axes(flux[0:1], flux[1:2], flux[2:3], tables)
    potential = dn_own - (div_x[0] + div_y[0] + div_z[0])
    return potential[None]


def solution(mesh):
    in_specs = (P("spin", "band", "grid", None, None), P("spin", None), P("grid", None, None))
    out_specs = P("spin", "grid", "band", None)
    return jax.shard_map(
        per_device, mesh=mesh, in_specs=in_specs, out_specs=out_specs, check_vma=False
    )
```

```python
import functools
import math

import jax
import jax.numpy as jnp
import numpy as np
from jax import lax
from jax.experimental import pallas as pl
from jax.experimental.pallas import tpu as pltpu
from jax.sharding import PartitionSpec as P

KAPPA = 0.804
MU_X = 0.2195149727645171
BETA = 0.06672455060314922
GAMMA = (1.0 - math.log(2.0)) / math.pi**2
FZ_NORM = 2.0 ** (4.0 / 3.0) - 2.0
FPP_ZERO = 1.709921
EXACT = lax.Precision.HIGHEST
MESH = pl.DeviceIdType.MESH
CHUNK = 4
FAST = 2
STEPS = 2
PARTS = 4
XC_ROWS = 2


def cube_root(value):
    return jnp.exp(jnp.log(value) * (1.0 / 3.0))


def pw_fit(radius, root, amp, alpha, beta_one, beta_two, beta_three, beta_four):
    denom = (2.0 * amp) * (
        root * (beta_one + root * (beta_two + root * (beta_three + root * beta_four)))
    )
    return -2.0 * amp * (1.0 + alpha * radius) * jnp.log(1.0 + 1.0 / denom)


def exchange_part(double, sigma_four):
    kfermi = (3.0 * math.pi**2) ** (1.0 / 3.0) * cube_root(double)
    product = kfermi * double
    scaled = sigma_four / (4.0 * product * product)
    enhance = 1.0 + KAPPA - KAPPA / (1.0 + MU_X * scaled / KAPPA)
    return -0.75 / math.pi * product * enhance


def xc_energy(n_up, n_down, s_uu, s_ud, s_dd):
    exch = 0.5 * (exchange_part(2.0 * n_up, 4.0 * s_uu) + exchange_part(2.0 * n_down, 4.0 * s_dd))
    total = n_up + n_down
    zeta = (n_up - n_down) / total
    third = cube_root(total)
    radius = (3.0 / (4.0 * math.pi)) ** (1.0 / 3.0) / third
    root = jnp.sqrt(radius)
    ec_para = pw_fit(radius, root, 0.031091, 0.2137, 7.5957, 3.5876, 1.6382, 0.49294)
    ec_ferro = pw_fit(radius, root, 0.015545, 0.20548, 14.1189, 6.1977, 3.3662, 0.62517)
    neg_stiff = pw_fit(radius, root, 0.016887, 0.11125, 10.357, 3.6231, 0.88026, 0.49671)
    plus_z = 1.0 + zeta
    minus_z = 1.0 - zeta
    plus_third = cube_root(plus_z)
    minus_third = cube_root(minus_z)
    fzeta = (plus_z * plus_third + minus_z * minus_third - 2.0) * (1.0 / FZ_NORM)
    zeta_sq = zeta * zeta
    zeta_four = zeta_sq * zeta_sq
    ec_lda = (
        ec_para
        - neg_stiff * fzeta * (1.0 / FPP_ZERO) * (1.0 - zeta_four)
        + (ec_ferro - ec_para) * fzeta * zeta_four
    )
    phi = 0.5 * (plus_third * plus_third + minus_third * minus_third)
    phi_cube = phi * phi * phi
    kfermi = (3.0 * math.pi**2) ** (1.0 / 3.0) * third
    screen_sq = kfermi * (4.0 / math.pi)
    sigma = s_uu + 2.0 * s_ud + s_dd
    tsq = sigma / (4.0 * phi * phi * screen_sq * total * total)
    amp = BETA / GAMMA / (jnp.exp(-ec_lda / (GAMMA * phi_cube)) - 1.0)
    atsq = amp * tsq
    gradient_term = (
        GAMMA
        * phi_cube
        * jnp.log(1.0 + BETA / GAMMA * tsq * (1.0 + atsq) / (1.0 + atsq + atsq * atsq))
    )
    return exch + total * (ec_lda + gradient_term)


def spectral_table(length):
    index = np.arange(length)
    angle = 2.0 * np.pi / length * (index[:, None] * index[None, :] % length)
    mode = np.where(index < length // 2, index, index - length)
    mode = np.where(index == length // 2, 0, mode)
    wave = 2.0 * np.pi / length * mode
    sines, cosines = np.sin(angle), np.cos(angle)
    first_term = (sines * wave[None, :]) @ cosines.T
    second_term = (cosines * wave[None, :]) @ sines.T
    return ((second_term - first_term) / length).astype(np.float32)


def greet(partners):
    barrier = pltpu.get_barrier_semaphore()
    for partner in partners:
        pl.semaphore_signal(barrier, inc=1, device_id=partner, device_id_type=MESH)
    pl.semaphore_wait(barrier, len(partners))


def density_kernel(
    bands,
    pairs_ref,
    orb_hbm,
    core_hbm,
    out_ref,
    orb,
    core,
    part,
    x_in,
    z_out,
    z_in,
    orb_sem,
    core_sem,
    x_send,
    x_recv,
    z_send,
    z_recv,
):
    count, rows, y_cells, z_cells = orb.shape
    block = core.shape[1]
    slow = bands // FAST
    chunks = rows // CHUNK
    me = lax.axis_index("band")
    my_slow, my_fast = lax.div(me, FAST), lax.rem(me, FAST)
    partner = {"band": my_slow * FAST + (1 - my_fast)}
    others = [{"band": lax.rem(my_slow + k, slow) * FAST + my_fast} for k in range(1, slow)]

    def orb_copy(c):
        span = pl.ds(c * CHUNK, CHUNK)
        return pltpu.make_async_copy(orb_hbm.at[0, :, span], orb.at[:, span], orb_sem.at[c])

    def core_copy():
        span = pl.ds(pl.multiple_of(me * block, block), block)
        return pltpu.make_async_copy(core_hbm.at[:, span], core, core_sem)

    def x_copy(c):
        span = pl.ds(c * CHUNK, CHUNK)
        return pltpu.make_async_remote_copy(
            src_ref=part.at[1 - my_fast, span],
            dst_ref=x_in.at[span],
            send_sem=x_send.at[c],
            recv_sem=x_recv.at[c],
            device_id=partner,
            device_id_type=MESH,
        )

    def z_copy(c, k):
        span = pl.ds(c * CHUNK, CHUNK)
        return pltpu.make_async_remote_copy(
            src_ref=z_out.at[lax.rem(my_slow + k, slow), span],
            dst_ref=z_in.at[k - 1, span],
            send_sem=z_send.at[k - 1, c],
            recv_sem=z_recv.at[k - 1, c],
            device_id=others[k - 1],
            device_id_type=MESH,
        )

    def each(body):
        lax.fori_loop(0, chunks, lambda c, carry: (body(c), carry)[1], 0)

    each(lambda c: orb_copy(c).start())
    core_copy().start()
    greet([partner] + others)
    first = pairs_ref[0, 0]
    last = first + pairs_ref[0, 1]
    weights = []
    for n in range(count):
        ident = me * count + n
        weights.append(jnp.where((ident >= first) & (ident < last), 0.5, 1.0).astype(jnp.float32))

    def density(c):
        orb_copy(c).wait()
        for r in range(CHUNK):
            row = c * CHUNK + r
            for piece in range(bands):
                total = jnp.zeros((block, z_cells), jnp.float32)
                for n in range(count):
                    values = orb[n, row, piece * block : (piece + 1) * block].astype(jnp.float32)
                    total += weights[n] * (values * values)
                part[piece % FAST, row, piece // FAST] = total
        x_copy(c).start()

    each(density)

    def forward(c):
        x_copy(c).wait_recv()
        span = pl.ds(c * CHUNK, CHUNK)
        for piece in range(slow):
            z_out[piece, span] = part[my_fast, span, piece] + x_in[span, piece]
        for k in range(1, slow):
            z_copy(c, k).start()

    each(forward)
    core_copy().wait()

    def collect(c):
        span = pl.ds(c * CHUNK, CHUNK)
        total = 0.5 * core[span] + z_out[my_slow, span]
        for k in range(1, slow):
            z_copy(c, k).wait_recv()
            total += z_in[k - 1, span]
        out_ref[span] = total

    each(collect)

    def drain(c):
        x_copy(c).wait_send()
        for k in range(1, slow):
            z_copy(c, k).wait_send()

    each(drain)


def own_density(orbitals, partial_bands, core_density):
    bands = lax.axis_size("band")
    _, count, rows, y_cells, z_cells = orbitals.shape
    block = y_cells // bands
    slow = bands // FAST
    chunks = rows // CHUNK
    return pl.pallas_call(
        functools.partial(density_kernel, bands),
        out_shape=jax.ShapeDtypeStruct((rows, block, z_cells), jnp.float32),
        in_specs=[
            pl.BlockSpec(memory_space=pltpu.SMEM),
            pl.BlockSpec(memory_space=pl.ANY),
            pl.BlockSpec(memory_space=pl.ANY),
        ],
        out_specs=pl.BlockSpec(memory_space=pltpu.VMEM),
        scratch_shapes=[
            pltpu.VMEM((count, rows, y_cells, z_cells), jnp.bfloat16),
            pltpu.VMEM((rows, block, z_cells), jnp.float32),
            pltpu.VMEM((FAST, rows, slow, block, z_cells), jnp.float32),
            pltpu.VMEM((rows, slow, block, z_cells), jnp.float32),
            pltpu.VMEM((slow, rows, block, z_cells), jnp.float32),
            pltpu.VMEM((slow - 1, rows, block, z_cells), jnp.float32),
            pltpu.SemaphoreType.DMA((chunks,)),
            pltpu.SemaphoreType.DMA,
            pltpu.SemaphoreType.DMA((chunks,)),
            pltpu.SemaphoreType.DMA((chunks,)),
            pltpu.SemaphoreType.DMA((slow - 1, chunks)),
            pltpu.SemaphoreType.DMA((slow - 1, chunks)),
        ],
        compiler_params=pltpu.CompilerParams(
            collective_id=0, has_side_effects=True, vmem_limit_bytes=48 * 2**20
        ),
        name="band_density",
    )(partial_bands, orbitals, core_density)


def field_kernel(
    bands,
    grids,
    own_ref,
    tx_ref,
    ty_ref,
    tz_ref,
    out_ref,
    line,
    gx,
    hx,
    sx,
    gy,
    hy,
    sy,
    dx,
    dz,
    other,
    fields,
    outgoing,
    xf_send,
    xf_recv,
    xb_send,
    xb_recv,
    yf_send,
    yf_recv,
    yb_send,
    yb_recv,
    in_send,
    in_recv,
    out_send,
    out_recv,
):
    rows, block, z_cells = own_ref.shape
    y_part = block // grids
    r_part = rows // bands
    steps = yf_send.shape[1]
    r_step = r_part // steps
    half = rows // 2
    parts = out_send.shape[0]
    p_rows = half // parts
    me = lax.axis_index("band")
    slab = lax.axis_index("grid")
    spin = lax.axis_index("spin")
    twin = {"spin": 1 - spin}
    my_block = pl.ds(pl.multiple_of(me * block, 8), block)
    my_slab = pl.ds(pl.multiple_of(slab * rows, 8), rows)
    mine = pl.ds(spin * half, half)
    theirs = pl.ds((1 - spin) * half, half)

    def remote(src, dst, send, recv, device):
        return pltpu.make_async_remote_copy(
            src_ref=src,
            dst_ref=dst,
            send_sem=send,
            recv_sem=recv,
            device_id=device,
            device_id_type=MESH,
        )

    def x_forward(t, k):
        q = lax.rem(slab + k, grids)
        return remote(
            line.at[t, pl.ds(q * y_part, y_part)],
            gx.at[t, :, my_slab],
            xf_send.at[t, k - 1],
            xf_recv.at[t, k - 1],
            {"grid": q},
        )

    def x_back(t, k):
        q = lax.rem(slab + k, grids)
        return remote(
            hx.at[t, :, pl.ds(pl.multiple_of(q * rows, 8), rows)],
            sx.at[t, pl.ds(slab * y_part, y_part)],
            xb_send.at[t, k - 1],
            xb_recv.at[t, k - 1],
            {"grid": q},
        )

    def y_forward(t, s, k):
        q = lax.rem(me + k, bands)
        source = own_ref if t == 0 else fields.at[2]
        return remote(
            source.at[pl.ds(q * r_part + s * r_step, r_step)],
            gy.at[t, pl.ds(s * r_step, r_step), my_block],
            yf_send.at[t, s, k - 1],
            yf_recv.at[t, s, k - 1],
            {"band": q},
        )

    def y_back(t, s, k):
        q = lax.rem(me + k, bands)
        return remote(
            hy.at[t, pl.ds(s * r_step, r_step), pl.ds(pl.multiple_of(q * block, 8), block)],
            sy.at[t, pl.ds(me * r_part + s * r_step, r_step)],
            yb_send.at[t, s, k - 1],
            yb_recv.at[t, s, k - 1],
            {"band": q},
        )

    incoming = [own_ref, dz, dx, sy.at[0]]

    def swap_in(f):
        return remote(
            incoming[f].at[theirs], other.at[f], in_send.at[f], in_recv.at[f], twin
        )

    def swap_out(p):
        return remote(
            outgoing.at[:, pl.ds(p * p_rows, p_rows)],
            fields.at[:, pl.ds(spin * half + p * p_rows, p_rows)],
            out_send.at[p],
            out_recv.at[p],
            twin,
        )

    def times(table, field):
        return jnp.dot(table, field, precision=EXACT, preferred_element_type=jnp.float32)

    def turned(value):
        return jnp.transpose(value, (1, 0, 2))

    def along_third(field):
        flat = field.reshape(rows * block, z_cells)
        return times(flat, tz_ref[...]).reshape(rows, block, z_cells)

    def start(t):
        for s in range(steps):
            for k in range(1, bands):
                y_forward(t, s, k).start()
        source = own_ref if t == 0 else fields.at[1]
        line[t] = turned(source[...])
        for k in range(1, grids):
            x_forward(t, k).start()
        gx[t, :, my_slab] = line[t, pl.ds(slab * y_part, y_part)]
        y_source = own_ref if t == 0 else fields.at[2]
        gy[t, :, my_block] = y_source[pl.ds(me * r_part, r_part)]

    def along_first(t):
        for k in range(1, grids):
            x_forward(t, k).wait_recv()
        for y in range(y_part):
            hx[t, y] = times(tx_ref[...], gx[t, y])
        for k in range(1, grids):
            x_back(t, k).start()
        sx[t, pl.ds(slab * y_part, y_part)] = hx[t, :, my_slab]

    def along_second(t):
        for s in range(steps):
            for k in range(1, bands):
                y_forward(t, s, k).wait_recv()
            for r in range(s * r_step, (s + 1) * r_step):
                hy[t, r] = times(ty_ref[...], gy[t, r])
            for k in range(1, bands):
                y_back(t, s, k).start()
        sy[t, pl.ds(me * r_part, r_part)] = hy[t, :, my_block]

    def end_first(t):
        for k in range(1, grids):
            x_back(t, k).wait_recv()
        return turned(sx[t])

    def end_second(t):
        for s in range(steps):
            for k in range(1, bands):
                y_back(t, s, k).wait_recv()

    greet(
        [twin]
        + [{"grid": lax.rem(slab + k, grids)} for k in range(1, grids)]
        + [{"band": lax.rem(me + k, bands)} for k in range(1, bands)]
    )
    start(0)
    swap_in(0).start()
    dz[...] = along_third(own_ref[...])
    swap_in(1).start()
    along_first(0)
    along_second(0)
    dx[...] = end_first(0)
    swap_in(2).start()
    end_second(0)
    swap_in(3).start()
    for f in range(4):
        swap_in(f).wait_recv()

    def potential_rows(row):
        here = pl.ds(spin * half + row, XC_ROWS)
        there = pl.ds(row, XC_ROWS)
        n_own, n_other = own_ref[here], other[0, there]
        g_own = [dx[here], sy[0, here], dz[here]]
        g_other = [other[2, there], other[3, there], other[1, there]]
        s_own = g_own[0] * g_own[0] + g_own[1] * g_own[1] + g_own[2] * g_own[2]
        s_mix = g_own[0] * g_other[0] + g_own[1] * g_other[1] + g_own[2] * g_other[2]
        s_other = g_other[0] * g_other[0] + g_other[1] * g_other[1] + g_other[2] * g_other[2]
        energy, pull = jax.vjp(xc_energy, n_own, n_other, s_own, s_mix, s_other)
        derivs = pull(jnp.ones_like(energy))
        fields[0, here] = derivs[0]
        outgoing[0, there] = derivs[1]
        for a in range(3):
            fields[1 + a, here] = 2.0 * derivs[2] * g_own[a] + derivs[3] * g_other[a]
            outgoing[1 + a, there] = 2.0 * derivs[4] * g_other[a] + derivs[3] * g_own[a]

    for p in range(parts):
        lax.fori_loop(
            0,
            p_rows // XC_ROWS,
            lambda i, carry: (potential_rows(p * p_rows + i * XC_ROWS), carry)[1],
            0,
        )
        swap_out(p).start()
    for p in range(parts):
        swap_out(p).wait_recv()
    start(1)
    along_first(1)
    out_ref[...] = fields[0] - along_third(fields[3])
    along_second(1)
    first = end_first(1)
    end_second(1)
    out_ref[...] = out_ref[...] - (first + sy[1])

    for t in range(2):
        for k in range(1, grids):
            x_forward(t, k).wait_send()
            x_back(t, k).wait_send()
        for s in range(steps):
            for k in range(1, bands):
                y_forward(t, s, k).wait_send()
                y_back(t, s, k).wait_send()
    for f in range(4):
        swap_in(f).wait_send()
    for p in range(parts):
        swap_out(p).wait_send()


def field_potential(own, tables):
    bands, grids = lax.axis_size("band"), lax.axis_size("grid")
    rows, block, z_cells = own.shape
    y_part, r_part = block // grids, rows // bands
    y_cells, x_cells = block * bands, rows * grids
    steps = math.gcd(STEPS, r_part)
    parts = math.gcd(PARTS, rows // 2 // XC_ROWS)
    vmem = pl.BlockSpec(memory_space=pltpu.VMEM)
    dma = pltpu.SemaphoreType.DMA
    real = jnp.float32
    return pl.pallas_call(
        functools.partial(field_kernel, bands, grids),
        out_shape=jax.ShapeDtypeStruct((rows, block, z_cells), real),
        in_specs=[vmem] * 4,
        out_specs=vmem,
        scratch_shapes=[
            pltpu.VMEM((2, block, rows, z_cells), real),
            pltpu.VMEM((2, y_part, x_cells, z_cells), real),
            pltpu.VMEM((2, y_part, x_cells, z_cells), real),
            pltpu.VMEM((2, block, rows, z_cells), real),
            pltpu.VMEM((2, r_part, y_cells, z_cells), real),
            pltpu.VMEM((2, r_part, y_cells, z_cells), real),
            pltpu.VMEM((2, rows, block, z_cells), real),
            pltpu.VMEM((rows, block, z_cells), real),
            pltpu.VMEM((rows, block, z_cells), real),
            pltpu.VMEM((4, rows // 2, block, z_cells), real),
            pltpu.VMEM((4, rows, block, z_cells), real),
            pltpu.VMEM((4, rows // 2, block, z_cells), real),
        ]
        + [dma((2, grids - 1))] * 4
        + [dma((2, steps, bands - 1))] * 4
        + [dma((4,))] * 2
        + [dma((parts,))] * 2,
        compiler_params=pltpu.CompilerParams(
            collective_id=1, has_side_effects=True, vmem_limit_bytes=32 * 2**20
        ),
        name="field_potential",
    )(own, *tables)


def per_device(orbitals, partial_bands, core_density):
    x_rows, y_cols, z_cells = core_density.shape
    tables = (
        jnp.asarray(spectral_table(x_rows * lax.axis_size("grid"))),
        jnp.asarray(spectral_table(y_cols)),
        jnp.asarray(spectral_table(z_cells).T),
    )
    own = own_density(orbitals, partial_bands, core_density)
    return field_potential(own, tables)[None]


def solution(mesh):
    in_specs = (P("spin", "band", "grid", None, None), P("spin", None), P("grid", None, None))
    out_specs = P("spin", "grid", "band", None)
    return jax.shard_map(
        per_device, mesh=mesh, in_specs=in_specs, out_specs=out_specs, check_vma=False
    )
```

```python
import functools
import math

import jax
import jax.numpy as jnp
import numpy as np
from jax import lax
from jax.experimental import pallas as pl
from jax.experimental.pallas import tpu as pltpu
from jax.sharding import PartitionSpec as P

KAPPA = 0.804
MU_X = 0.2195149727645171
BETA = 0.06672455060314922
GAMMA = (1.0 - math.log(2.0)) / math.pi**2
FZ_NORM = 2.0 ** (4.0 / 3.0) - 2.0
FPP_ZERO = 1.709921
EXACT = lax.Precision.HIGHEST
MESH = pl.DeviceIdType.MESH
CHUNK = 4
FAST = 2
XC_ROWS = 2
TILE = 8


def cube_root(value):
    return jnp.exp(jnp.log(value) * (1.0 / 3.0))


def pw_fit(radius, root, amp, alpha, beta_one, beta_two, beta_three, beta_four):
    denom = (2.0 * amp) * (
        root * (beta_one + root * (beta_two + root * (beta_three + root * beta_four)))
    )
    return -2.0 * amp * (1.0 + alpha * radius) * jnp.log(1.0 + 1.0 / denom)


def exchange_part(double, sigma_four):
    kfermi = (3.0 * math.pi**2) ** (1.0 / 3.0) * cube_root(double)
    product = kfermi * double
    scaled = sigma_four / (4.0 * product * product)
    enhance = 1.0 + KAPPA - KAPPA / (1.0 + MU_X * scaled / KAPPA)
    return -0.75 / math.pi * product * enhance


def xc_energy(n_up, n_down, s_uu, s_ud, s_dd):
    exch = 0.5 * (exchange_part(2.0 * n_up, 4.0 * s_uu) + exchange_part(2.0 * n_down, 4.0 * s_dd))
    total = n_up + n_down
    zeta = (n_up - n_down) / total
    third = cube_root(total)
    radius = (3.0 / (4.0 * math.pi)) ** (1.0 / 3.0) / third
    root = jnp.sqrt(radius)
    ec_para = pw_fit(radius, root, 0.031091, 0.2137, 7.5957, 3.5876, 1.6382, 0.49294)
    ec_ferro = pw_fit(radius, root, 0.015545, 0.20548, 14.1189, 6.1977, 3.3662, 0.62517)
    neg_stiff = pw_fit(radius, root, 0.016887, 0.11125, 10.357, 3.6231, 0.88026, 0.49671)
    plus_z = 1.0 + zeta
    minus_z = 1.0 - zeta
    plus_third = cube_root(plus_z)
    minus_third = cube_root(minus_z)
    fzeta = (plus_z * plus_third + minus_z * minus_third - 2.0) * (1.0 / FZ_NORM)
    zeta_sq = zeta * zeta
    zeta_four = zeta_sq * zeta_sq
    ec_lda = (
        ec_para
        - neg_stiff * fzeta * (1.0 / FPP_ZERO) * (1.0 - zeta_four)
        + (ec_ferro - ec_para) * fzeta * zeta_four
    )
    phi = 0.5 * (plus_third * plus_third + minus_third * minus_third)
    phi_cube = phi * phi * phi
    kfermi = (3.0 * math.pi**2) ** (1.0 / 3.0) * third
    screen_sq = kfermi * (4.0 / math.pi)
    sigma = s_uu + 2.0 * s_ud + s_dd
    tsq = sigma / (4.0 * phi * phi * screen_sq * total * total)
    amp = BETA / GAMMA / (jnp.exp(-ec_lda / (GAMMA * phi_cube)) - 1.0)
    atsq = amp * tsq
    gradient_term = (
        GAMMA
        * phi_cube
        * jnp.log(1.0 + BETA / GAMMA * tsq * (1.0 + atsq) / (1.0 + atsq + atsq * atsq))
    )
    return exch + total * (ec_lda + gradient_term)


def spectral_table(length):
    index = np.arange(length)
    angle = 2.0 * np.pi / length * (index[:, None] * index[None, :] % length)
    mode = np.where(index < length // 2, index, index - length)
    mode = np.where(index == length // 2, 0, mode)
    wave = 2.0 * np.pi / length * mode
    sines, cosines = np.sin(angle), np.cos(angle)
    first_term = (sines * wave[None, :]) @ cosines.T
    second_term = (cosines * wave[None, :]) @ sines.T
    return ((second_term - first_term) / length).astype(np.float32)


def greet(partners):
    barrier = pltpu.get_barrier_semaphore()
    for partner in partners:
        pl.semaphore_signal(barrier, inc=1, device_id=partner, device_id_type=MESH)
    pl.semaphore_wait(barrier, len(partners))


def potential_kernel(
    bands,
    grids,
    pairs_ref,
    orb_hbm,
    core_hbm,
    tx_ref,
    ty_ref,
    tz_ref,
    out_ref,
    orb,
    core,
    part,
    x_in,
    z_out,
    z_in,
    own,
    line,
    gx,
    hx,
    sx,
    gy,
    hy,
    sy,
    dx,
    dz,
    other,
    fields,
    outgoing,
    orb_sem,
    core_sem,
    x_send,
    x_recv,
    z_send,
    z_recv,
    xp_send,
    xp_recv,
    xf_send,
    xf_recv,
    xb_send,
    xb_recv,
    yf_send,
    yf_recv,
    yb_send,
    yb_recv,
    in_send,
    in_recv,
    gy_send,
    gy_recv,
    out_send,
    out_recv,
):
    count, rows, y_cells, z_cells = orb.shape
    block = core.shape[1]
    slow = bands // FAST
    steps = out_send.shape[0]
    r_part = rows // bands
    chunk = r_part // steps
    piece_rows = rows // xp_send.shape[0]
    pieces = rows // piece_rows
    per_piece = piece_rows // chunk
    chunks = rows // chunk
    y_part = block // grids
    half = bands // 2
    xc_rows = math.gcd(XC_ROWS, chunk)
    me = lax.axis_index("band")
    slab = lax.axis_index("grid")
    spin = lax.axis_index("spin")
    my_slow, my_fast = lax.div(me, FAST), lax.rem(me, FAST)
    partner = {"band": my_slow * FAST + (1 - my_fast)}
    others = [{"band": lax.rem(my_slow + k, slow) * FAST + my_fast} for k in range(1, slow)]
    twin = {"spin": 1 - spin}
    my_block = pl.ds(pl.multiple_of(me * block, TILE), block)
    my_slab = pl.ds(pl.multiple_of(slab * rows, TILE), rows)
    mine = pl.ds(spin * half, half)
    theirs = pl.ds((1 - spin) * half, half)

    def remote(src, dst, send, recv, device):
        return pltpu.make_async_remote_copy(
            src_ref=src,
            dst_ref=dst,
            send_sem=send,
            recv_sem=recv,
            device_id=device,
            device_id_type=MESH,
        )

    def orb_copy(u):
        span = pl.ds(u * piece_rows, piece_rows)
        return pltpu.make_async_copy(orb_hbm.at[0, :, span], orb.at[:, span], orb_sem.at[u])

    def core_copy():
        return pltpu.make_async_copy(core_hbm.at[:, my_block], core, core_sem)

    def x_copy(c):
        span = pl.ds(c * chunk, chunk)
        return remote(
            part.at[1 - my_fast, span], x_in.at[span], x_send.at[c], x_recv.at[c], partner
        )

    def z_copy(c, k):
        span = pl.ds(c * chunk, chunk)
        return remote(
            z_out.at[lax.rem(my_slow + k, slow), span],
            z_in.at[k - 1, span],
            z_send.at[k - 1, c],
            z_recv.at[k - 1, c],
            others[k - 1],
        )

    def x_piece(u, k):
        q = lax.rem(slab + k, grids)
        start = pl.multiple_of(u * piece_rows, TILE)
        there = pl.multiple_of(slab * rows + u * piece_rows, TILE)
        return remote(
            line.at[0, pl.ds(q * y_part, y_part), pl.ds(start, piece_rows)],
            gx.at[0, :, pl.ds(there, piece_rows)],
            xp_send.at[u, k - 1],
            xp_recv.at[u, k - 1],
            {"grid": q},
        )

    def x_whole(k):
        q = lax.rem(slab + k, grids)
        return remote(
            line.at[1, pl.ds(q * y_part, y_part)],
            gx.at[1, :, my_slab],
            xf_send.at[k - 1],
            xf_recv.at[k - 1],
            {"grid": q},
        )

    def x_back(t, k):
        q = lax.rem(slab + k, grids)
        return remote(
            hx.at[t, :, pl.ds(pl.multiple_of(q * rows, TILE), rows)],
            sx.at[t, pl.ds(slab * y_part, y_part)],
            xb_send.at[t, k - 1],
            xb_recv.at[t, k - 1],
            {"grid": q},
        )

    def y_forward(t, s, k):
        q = lax.rem(me + k, bands)
        source = own if t == 0 else fields.at[2]
        return remote(
            source.at[q, pl.ds(s * chunk, chunk)],
            gy.at[t, pl.ds(s * chunk, chunk), my_block],
            yf_send.at[t, s, k - 1],
            yf_recv.at[t, s, k - 1],
            {"band": q},
        )

    def y_back(t, s, k):
        q = lax.rem(me + k, bands)
        return remote(
            hy.at[t, pl.ds(s * chunk, chunk), pl.ds(pl.multiple_of(q * block, TILE), block)],
            sy.at[t, me, pl.ds(s * chunk, chunk)],
            yb_send.at[t, s, k - 1],
            yb_recv.at[t, s, k - 1],
            {"band": q},
        )

    incoming = [own, dz, dx]

    def swap_in(f):
        return remote(incoming[f].at[theirs], other.at[f], in_send.at[f], in_recv.at[f], twin)

    def swap_steep(s):
        span = pl.ds(s * chunk, chunk)
        return remote(
            sy.at[0, theirs, span], other.at[3, :, span], gy_send.at[s], gy_recv.at[s], twin
        )

    def swap_out(s):
        span = pl.ds(s * chunk, chunk)
        return remote(
            outgoing.at[:, :, span],
            fields.at[:, mine, span],
            out_send.at[s],
            out_recv.at[s],
            twin,
        )

    def times(table, field):
        return jnp.dot(table, field, precision=EXACT, preferred_element_type=jnp.float32)

    def turned(value):
        return jnp.transpose(value, (1, 0, 2))

    def whole(value):
        return value.reshape(rows, block, z_cells)

    def split(value):
        return value.reshape(bands, r_part, block, z_cells)

    def along_third(field):
        return times(field.reshape(rows * block, z_cells), tz_ref[...]).reshape(field.shape)

    def along_first(t):
        for y in range(y_part):
            hx[t, y] = times(tx_ref[...], gx[t, y])
        for k in range(1, grids):
            x_back(t, k).start()
        sx[t, pl.ds(slab * y_part, y_part)] = hx[t, :, my_slab]

    def along_second(t, s):
        for k in range(1, bands):
            y_forward(t, s, k).wait_recv()
        for r in range(s * chunk, (s + 1) * chunk):
            hy[t, r] = times(ty_ref[...], gy[t, r])
        for k in range(1, bands):
            y_back(t, s, k).start()
        span = pl.ds(s * chunk, chunk)
        sy[t, me, span] = hy[t, span, my_block]

    def end_first(t):
        for k in range(1, grids):
            x_back(t, k).wait_recv()
        return split(turned(sx[t]))

    def end_second(t, s):
        for k in range(1, bands):
            y_back(t, s, k).wait_recv()

    def each(number, body):
        lax.fori_loop(0, number, lambda i, carry: (body(i), carry)[1], 0)

    each(pieces, lambda u: orb_copy(u).start())
    core_copy().start()
    greet(
        [twin]
        + [{"grid": lax.rem(slab + k, grids)} for k in range(1, grids)]
        + [{"band": lax.rem(me + k, bands)} for k in range(1, bands)]
    )
    first = pairs_ref[0, 0]
    last = first + pairs_ref[0, 1]
    weights = []
    for n in range(count):
        ident = me * count + n
        weights.append(jnp.where((ident >= first) & (ident < last), 0.5, 1.0).astype(jnp.float32))

    def squares(u):
        orb_copy(u).wait()

        def one_chunk(i):
            c = u * per_piece + i
            for r in range(chunk):
                row = c * chunk + r
                for b in range(bands):
                    total = jnp.zeros((block, z_cells), jnp.float32)
                    for n in range(count):
                        values = orb[n, row, b * block : (b + 1) * block].astype(jnp.float32)
                        total += weights[n] * (values * values)
                    part[b % FAST, row, b // FAST] = total
            x_copy(c).start()

        each(per_piece, one_chunk)

    def forward(u):
        def one_chunk(i):
            c = u * per_piece + i
            x_copy(c).wait_recv()
            span = pl.ds(c * chunk, chunk)
            for d in range(slow):
                z_out[d, span] = part[my_fast, span, d] + x_in[span, d]
            for k in range(1, slow):
                z_copy(c, k).start()

        each(per_piece, one_chunk)

    def collect(u):
        def one_chunk(i):
            c = u * per_piece + i
            span = pl.ds(c * chunk, chunk)
            total = 0.5 * core[span] + z_out[my_slow, span]
            for k in range(1, slow):
                z_copy(c, k).wait_recv()
                total += z_in[k - 1, span]
            j, s = lax.div(c, steps), lax.rem(c, steps)
            own[j, pl.ds(s * chunk, chunk)] = total

            @pl.when(j != me)
            def _():
                y_forward(0, s, lax.rem(j - me + bands, bands)).start()

            @pl.when(j == me)
            def _():
                gy[0, pl.ds(s * chunk, chunk), my_block] = total

        each(per_piece, one_chunk)
        group = piece_rows // r_part
        rows_here = own[pl.ds(u * group, group)].reshape(piece_rows, block, z_cells)
        start = pl.multiple_of(u * piece_rows, TILE)
        there = pl.multiple_of(slab * rows + u * piece_rows, TILE)
        line[0, :, pl.ds(start, piece_rows)] = turned(rows_here)
        for k in range(1, grids):
            x_piece(u, k).start()
        gx[0, :, pl.ds(there, piece_rows)] = line[
            0, pl.ds(slab * y_part, y_part), pl.ds(start, piece_rows)
        ]

    squares(0)
    squares(1)
    core_copy().wait()

    def sum_step(u):
        forward(u)

        @pl.when(u + 2 < pieces)
        def _():
            squares(u + 2)

        @pl.when(u >= 1)
        def _():
            collect(u - 1)

    each(pieces, sum_step)
    collect(pieces - 1)

    swap_in(0).start()
    dz[...] = along_third(own[...])
    swap_in(1).start()
    along_second(0, 0)
    for u in range(pieces):
        for k in range(1, grids):
            x_piece(u, k).wait_recv()
    along_first(0)
    for s in range(1, steps):
        along_second(0, s)
    dx[...] = end_first(0)
    swap_in(2).start()
    for f in range(3):
        swap_in(f).wait()

    def potential_rows(j, row):
        span = pl.ds(row, xc_rows)
        here = (spin * half + j, span)
        there = (j, span)
        n_own, n_other = own[here], other[(0,) + there]
        g_own = [dx[here], sy[(0,) + here], dz[here]]
        g_other = [other[(2,) + there], other[(3,) + there], other[(1,) + there]]
        s_own = g_own[0] * g_own[0] + g_own[1] * g_own[1] + g_own[2] * g_own[2]
        s_mix = g_own[0] * g_other[0] + g_own[1] * g_other[1] + g_own[2] * g_other[2]
        s_other = g_other[0] * g_other[0] + g_other[1] * g_other[1] + g_other[2] * g_other[2]
        energy, pull = jax.vjp(xc_energy, n_own, n_other, s_own, s_mix, s_other)
        derivs = pull(jnp.ones_like(energy))
        fields[(0,) + here] = derivs[0]
        outgoing[(0,) + there] = derivs[1]
        for a in range(3):
            fields[(1 + a,) + here] = 2.0 * derivs[2] * g_own[a] + derivs[3] * g_other[a]
            outgoing[(1 + a,) + there] = 2.0 * derivs[4] * g_other[a] + derivs[3] * g_own[a]

    def flux_out(s):
        swap_out(s).wait_recv()
        for k in range(1, bands):
            y_forward(1, s, k).start()
        span = pl.ds(s * chunk, chunk)
        gy[1, span, my_block] = fields[2, me, span]

    end_second(0, 0)
    swap_steep(0).start()
    for s in range(steps):
        swap_steep(s).wait_recv()
        per_group = chunk // xc_rows
        each(
            half * per_group,
            lambda i: potential_rows(
                lax.div(i, per_group), s * chunk + lax.rem(i, per_group) * xc_rows
            ),
        )
        swap_out(s).start()
        if s + 1 < steps:
            end_second(0, s + 1)
            swap_steep(s + 1).start()
        flux_out(s)

    line[1] = turned(whole(fields[1]))
    for k in range(1, grids):
        x_whole(k).start()
    gx[1, :, my_slab] = line[1, pl.ds(slab * y_part, y_part)]
    for s in range(steps - 1):
        along_second(1, s)
    dz[...] = fields[0] - along_third(fields[3])
    for k in range(1, grids):
        x_whole(k).wait_recv()
    along_first(1)
    along_second(1, steps - 1)
    dz[...] = dz[...] - end_first(1)
    for s in range(steps):
        end_second(1, s)
    out_ref[...] = whole(dz[...] - sy[1])

    def drain(c):
        x_copy(c).wait_send()
        for k in range(1, slow):
            z_copy(c, k).wait_send()

    each(chunks, drain)
    for k in range(1, grids):
        for u in range(pieces):
            x_piece(u, k).wait_send()
        x_whole(k).wait_send()
        x_back(0, k).wait_send()
        x_back(1, k).wait_send()
    for t in range(2):
        for s in range(steps):
            for k in range(1, bands):
                y_forward(t, s, k).wait_send()
                y_back(t, s, k).wait_send()
    for s in range(steps):
        swap_steep(s).wait_send()
        swap_out(s).wait_send()


def potential_call(orbitals, partial_bands, core_density, tables):
    bands, grids = lax.axis_size("band"), lax.axis_size("grid")
    _, count, rows, y_cells, z_cells = orbitals.shape
    block, slow = y_cells // bands, bands // FAST
    y_part, r_part = block // grids, rows // bands
    x_cells = rows * grids
    steps = r_part // math.gcd(CHUNK, r_part)
    chunks = bands * steps
    pieces = rows // max(r_part, TILE)
    half = bands // 2
    vmem = pl.BlockSpec(memory_space=pltpu.VMEM)
    hbm = pl.BlockSpec(memory_space=pl.ANY)
    dma = pltpu.SemaphoreType.DMA
    real = jnp.float32
    cells = (bands, r_part, block, z_cells)
    return pl.pallas_call(
        functools.partial(potential_kernel, bands, grids),
        out_shape=jax.ShapeDtypeStruct((rows, block, z_cells), real),
        in_specs=[pl.BlockSpec(memory_space=pltpu.SMEM), hbm, hbm] + [vmem] * 3,
        out_specs=vmem,
        scratch_shapes=[
            pltpu.VMEM((count, rows, y_cells, z_cells), jnp.bfloat16),
            pltpu.VMEM((rows, block, z_cells), real),
            pltpu.VMEM((FAST, rows, slow, block, z_cells), real),
            pltpu.VMEM((rows, slow, block, z_cells), real),
            pltpu.VMEM((slow, rows, block, z_cells), real),
            pltpu.VMEM((slow - 1, rows, block, z_cells), real),
            pltpu.VMEM(cells, real),
            pltpu.VMEM((2, block, rows, z_cells), real),
            pltpu.VMEM((2, y_part, x_cells, z_cells), real),
            pltpu.VMEM((2, y_part, x_cells, z_cells), real),
            pltpu.VMEM((2, block, rows, z_cells), real),
            pltpu.VMEM((2, r_part, y_cells, z_cells), real),
            pltpu.VMEM((2, r_part, y_cells, z_cells), real),
            pltpu.VMEM((2,) + cells, real),
            pltpu.VMEM(cells, real),
            pltpu.VMEM(cells, real),
            pltpu.VMEM((4, half) + cells[1:], real),
            pltpu.VMEM((4,) + cells, real),
            pltpu.VMEM((4, half) + cells[1:], real),
            dma((pieces,)),
            dma,
            dma((chunks,)),
            dma((chunks,)),
            dma((slow - 1, chunks)),
            dma((slow - 1, chunks)),
        ]
        + [dma((pieces, grids - 1))] * 2
        + [dma((grids - 1,))] * 2
        + [dma((2, grids - 1))] * 2
        + [dma((2, steps, bands - 1))] * 4
        + [dma((3,))] * 2
        + [dma((steps,))] * 4,
        compiler_params=pltpu.CompilerParams(
            collective_id=0, has_side_effects=True, vmem_limit_bytes=60 * 2**20
        ),
        name="potential",
    )(partial_bands, orbitals, core_density, *tables)


def per_device(orbitals, partial_bands, core_density):
    x_rows, y_cols, z_cells = core_density.shape
    tables = (
        jnp.asarray(spectral_table(x_rows * lax.axis_size("grid"))),
        jnp.asarray(spectral_table(y_cols)),
        jnp.asarray(spectral_table(z_cells).T),
    )
    return potential_call(orbitals, partial_bands, core_density, tables)[None]


def solution(mesh):
    in_specs = (P("spin", "band", "grid", None, None), P("spin", None), P("grid", None, None))
    out_specs = P("spin", "grid", "band", None)
    return jax.shard_map(
        per_device, mesh=mesh, in_specs=in_specs, out_specs=out_specs, check_vma=False
    )
```

```python
import functools
import math

import jax
import jax.numpy as jnp
import numpy as np
from jax import lax
from jax.experimental import pallas as pl
from jax.experimental.pallas import tpu as pltpu
from jax.sharding import PartitionSpec as P

KAPPA = 0.804
MU_X = 0.2195149727645171
BETA = 0.06672455060314922
GAMMA = (1.0 - math.log(2.0)) / math.pi**2
FZ_NORM = 2.0 ** (4.0 / 3.0) - 2.0
FPP_ZERO = 1.709921
EXACT = lax.Precision.HIGHEST
MESH = pl.DeviceIdType.MESH
CHUNK = 4
FAST = 2
XC_ROWS = 2
TILE = 8


def cube_root(value):
    return jnp.exp(jnp.log(value) * (1.0 / 3.0))


def pw_fit(radius, root, amp, alpha, beta_one, beta_two, beta_three, beta_four):
    denom = (2.0 * amp) * (
        root * (beta_one + root * (beta_two + root * (beta_three + root * beta_four)))
    )
    return -2.0 * amp * (1.0 + alpha * radius) * jnp.log(1.0 + 1.0 / denom)


def exchange_part(double, sigma_four):
    kfermi = (3.0 * math.pi**2) ** (1.0 / 3.0) * cube_root(double)
    product = kfermi * double
    scaled = sigma_four / (4.0 * product * product)
    enhance = 1.0 + KAPPA - KAPPA / (1.0 + MU_X * scaled / KAPPA)
    return -0.75 / math.pi * product * enhance


def xc_energy(n_up, n_down, s_uu, s_ud, s_dd):
    exch = 0.5 * (exchange_part(2.0 * n_up, 4.0 * s_uu) + exchange_part(2.0 * n_down, 4.0 * s_dd))
    total = n_up + n_down
    zeta = (n_up - n_down) / total
    third = cube_root(total)
    radius = (3.0 / (4.0 * math.pi)) ** (1.0 / 3.0) / third
    root = jnp.sqrt(radius)
    ec_para = pw_fit(radius, root, 0.031091, 0.2137, 7.5957, 3.5876, 1.6382, 0.49294)
    ec_ferro = pw_fit(radius, root, 0.015545, 0.20548, 14.1189, 6.1977, 3.3662, 0.62517)
    neg_stiff = pw_fit(radius, root, 0.016887, 0.11125, 10.357, 3.6231, 0.88026, 0.49671)
    plus_z = 1.0 + zeta
    minus_z = 1.0 - zeta
    plus_third = cube_root(plus_z)
    minus_third = cube_root(minus_z)
    fzeta = (plus_z * plus_third + minus_z * minus_third - 2.0) * (1.0 / FZ_NORM)
    zeta_sq = zeta * zeta
    zeta_four = zeta_sq * zeta_sq
    ec_lda = (
        ec_para
        - neg_stiff * fzeta * (1.0 / FPP_ZERO) * (1.0 - zeta_four)
        + (ec_ferro - ec_para) * fzeta * zeta_four
    )
    phi = 0.5 * (plus_third * plus_third + minus_third * minus_third)
    phi_cube = phi * phi * phi
    kfermi = (3.0 * math.pi**2) ** (1.0 / 3.0) * third
    screen_sq = kfermi * (4.0 / math.pi)
    sigma = s_uu + 2.0 * s_ud + s_dd
    tsq = sigma / (4.0 * phi * phi * screen_sq * total * total)
    amp = BETA / GAMMA / (jnp.exp(-ec_lda / (GAMMA * phi_cube)) - 1.0)
    atsq = amp * tsq
    gradient_term = (
        GAMMA
        * phi_cube
        * jnp.log(1.0 + BETA / GAMMA * tsq * (1.0 + atsq) / (1.0 + atsq + atsq * atsq))
    )
    return exch + total * (ec_lda + gradient_term)


def spectral_table(length):
    index = np.arange(length)
    angle = 2.0 * np.pi / length * (index[:, None] * index[None, :] % length)
    mode = np.where(index < length // 2, index, index - length)
    mode = np.where(index == length // 2, 0, mode)
    wave = 2.0 * np.pi / length * mode
    sines, cosines = np.sin(angle), np.cos(angle)
    first_term = (sines * wave[None, :]) @ cosines.T
    second_term = (cosines * wave[None, :]) @ sines.T
    return ((second_term - first_term) / length).astype(np.float32)


def potential_kernel(
    bands,
    grids,
    pairs_ref,
    orb_hbm,
    core_hbm,
    tx_ref,
    ty_ref,
    tz_ref,
    out_ref,
    orb,
    core,
    part,
    x_in,
    z_out,
    p_in,
    w_out,
    w_in,
    own,
    line,
    gx,
    hx,
    sx,
    gy,
    hy,
    sy,
    dx,
    dz,
    other,
    fields,
    outgoing,
    orb_sem,
    core_sem,
    x_send,
    x_recv,
    p_send,
    p_recv,
    w_send,
    w_recv,
    xp_send,
    xp_recv,
    xf_send,
    xf_recv,
    xb_send,
    xb_recv,
    yf_send,
    yf_recv,
    yb_send,
    yb_recv,
    in_send,
    in_recv,
    gy_send,
    gy_recv,
    out_send,
    out_recv,
):
    count, rows, y_cells, z_cells = orb.shape
    block = core.shape[1]
    slow = bands // FAST
    steps = out_send.shape[0]
    r_part = rows // bands
    chunk = r_part // steps
    piece_rows = rows // xp_send.shape[0]
    pieces = rows // piece_rows
    per_piece = piece_rows // chunk
    chunks = rows // chunk
    y_part = block // grids
    half = bands // 2
    xc_rows = math.gcd(XC_ROWS, chunk)
    me = lax.axis_index("band")
    slab = lax.axis_index("grid")
    spin = lax.axis_index("spin")
    my_slow, my_fast = lax.div(me, FAST), lax.rem(me, FAST)
    partner = {"band": my_slow * FAST + (1 - my_fast)}
    pairs = slow // 2
    my_pair = lax.div(my_slow, 2)
    my_kind = lax.rem(my_slow + my_pair, 2)
    beside = {"band": (my_slow + 1 - 2 * lax.rem(my_slow, 2)) * FAST + my_fast}
    twin = {"spin": 1 - spin}
    my_block = pl.ds(pl.multiple_of(me * block, TILE), block)
    my_slab = pl.ds(pl.multiple_of(slab * rows, TILE), rows)
    mine = pl.ds(spin * half, half)
    theirs = pl.ds((1 - spin) * half, half)

    def remote(src, dst, send, recv, device):
        return pltpu.make_async_remote_copy(
            src_ref=src,
            dst_ref=dst,
            send_sem=send,
            recv_sem=recv,
            device_id=device,
            device_id_type=MESH,
        )

    def orb_copy(u):
        span = pl.ds(u * piece_rows, piece_rows)
        return pltpu.make_async_copy(orb_hbm.at[0, :, span], orb.at[:, span], orb_sem.at[u])

    def core_copy():
        return pltpu.make_async_copy(core_hbm.at[:, my_block], core, core_sem)

    def x_copy(c):
        span = pl.ds(c * chunk, chunk)
        return remote(
            part.at[1 - my_fast, span], x_in.at[span], x_send.at[c], x_recv.at[c], partner
        )

    def pair_copy(c):
        span = pl.ds(c * chunk, chunk)
        return remote(
            z_out.at[1 - my_kind, :, span],
            p_in.at[:, span],
            p_send.at[c],
            p_recv.at[c],
            beside,
        )

    def z_copy(c, k):
        span = pl.ds(c * chunk, chunk)
        h = lax.rem(my_pair + k, pairs)
        return remote(
            w_out.at[h, span],
            w_in.at[k - 1, span],
            w_send.at[k - 1, c],
            w_recv.at[k - 1, c],
            {"band": (2 * h + lax.rem(my_kind + h, 2)) * FAST + my_fast},
        )

    def x_piece(u, k):
        q = lax.rem(slab + k, grids)
        start = pl.multiple_of(u * piece_rows, TILE)
        there = pl.multiple_of(slab * rows + u * piece_rows, TILE)
        return remote(
            line.at[0, pl.ds(q * y_part, y_part), pl.ds(start, piece_rows)],
            gx.at[0, :, pl.ds(there, piece_rows)],
            xp_send.at[u, k - 1],
            xp_recv.at[u, k - 1],
            {"grid": q},
        )

    def x_whole(k):
        q = lax.rem(slab + k, grids)
        return remote(
            line.at[1, pl.ds(q * y_part, y_part)],
            gx.at[1, :, my_slab],
            xf_send.at[k - 1],
            xf_recv.at[k - 1],
            {"grid": q},
        )

    def x_back(t, k):
        q = lax.rem(slab + k, grids)
        return remote(
            hx.at[t, :, pl.ds(pl.multiple_of(q * rows, TILE), rows)],
            sx.at[t, pl.ds(slab * y_part, y_part)],
            xb_send.at[t, k - 1],
            xb_recv.at[t, k - 1],
            {"grid": q},
        )

    def y_forward(t, s, k):
        q = lax.rem(me + k, bands)
        source = own if t == 0 else fields.at[2]
        return remote(
            source.at[q, pl.ds(s * chunk, chunk)],
            gy.at[t, pl.ds(s * chunk, chunk), my_block],
            yf_send.at[t, s, k - 1],
            yf_recv.at[t, s, k - 1],
            {"band": q},
        )

    def y_back(t, s, k):
        q = lax.rem(me + k, bands)
        return remote(
            hy.at[t, pl.ds(s * chunk, chunk), pl.ds(pl.multiple_of(q * block, TILE), block)],
            sy.at[t, me, pl.ds(s * chunk, chunk)],
            yb_send.at[t, s, k - 1],
            yb_recv.at[t, s, k - 1],
            {"band": q},
        )

    incoming = [own, dz, dx]

    def swap_in(f):
        return remote(incoming[f].at[theirs], other.at[f], in_send.at[f], in_recv.at[f], twin)

    def swap_steep(s):
        span = pl.ds(s * chunk, chunk)
        return remote(
            sy.at[0, theirs, span], other.at[3, :, span], gy_send.at[s], gy_recv.at[s], twin
        )

    def swap_out(s):
        span = pl.ds(s * chunk, chunk)
        return remote(
            outgoing.at[:, :, span],
            fields.at[:, mine, span],
            out_send.at[s],
            out_recv.at[s],
            twin,
        )

    def times(table, field):
        return jnp.dot(table, field, precision=EXACT, preferred_element_type=jnp.float32)

    def turned(value):
        return jnp.transpose(value, (1, 0, 2))

    def whole(value):
        return value.reshape(rows, block, z_cells)

    def split(value):
        return value.reshape(bands, r_part, block, z_cells)

    def along_third(field):
        return times(field.reshape(rows * block, z_cells), tz_ref[...]).reshape(field.shape)

    def along_first(t):
        for y in range(y_part):
            hx[t, y] = times(tx_ref[...], gx[t, y])
        for k in range(1, grids):
            x_back(t, k).start()
        sx[t, pl.ds(slab * y_part, y_part)] = hx[t, :, my_slab]

    def along_second(t, s):
        for k in range(1, bands):
            y_forward(t, s, k).wait_recv()
        for r in range(s * chunk, (s + 1) * chunk):
            hy[t, r] = times(ty_ref[...], gy[t, r])
        for k in range(1, bands):
            y_back(t, s, k).start()
        span = pl.ds(s * chunk, chunk)
        sy[t, me, span] = hy[t, span, my_block]

    def end_first(t):
        for k in range(1, grids):
            x_back(t, k).wait_recv()
        return split(turned(sx[t]))

    def end_second(t, s):
        for k in range(1, bands):
            y_back(t, s, k).wait_recv()

    def each(number, body):
        lax.fori_loop(0, number, lambda i, carry: (body(i), carry)[1], 0)

    each(pieces, lambda u: orb_copy(u).start())
    core_copy().start()
    partners = (
        [twin]
        + [{"grid": lax.rem(slab + k, grids)} for k in range(1, grids)]
        + [{"band": lax.rem(me + k, bands)} for k in range(1, bands)]
    )
    barrier = pltpu.get_barrier_semaphore()
    for target in partners:
        pl.semaphore_signal(barrier, inc=1, device_id=target, device_id_type=MESH)
    first = pairs_ref[0, 0]
    last = first + pairs_ref[0, 1]
    weights = []
    for n in range(count):
        ident = me * count + n
        weights.append(jnp.where((ident >= first) & (ident < last), 0.5, 1.0).astype(jnp.float32))

    def squares(u):
        orb_copy(u).wait()

        def one_chunk(i):
            c = u * per_piece + i
            for r in range(chunk):
                row = c * chunk + r
                for b in range(bands):
                    total = jnp.zeros((block, z_cells), jnp.float32)
                    for n in range(count):
                        values = orb[n, row, b * block : (b + 1) * block].astype(jnp.float32)
                        total += weights[n] * (values * values)
                    part[b % FAST, row, b // FAST] = total

        each(per_piece, one_chunk)

    def send_squares(u):
        each(per_piece, lambda i: x_copy(u * per_piece + i).start())

    def forward(u):
        def one_chunk(i):
            c = u * per_piece + i
            x_copy(c).wait_recv()
            span = pl.ds(c * chunk, chunk)
            for d in range(slow):
                z_out[(d + d // 2) % 2, d // 2, span] = part[my_fast, span, d] + x_in[span, d]
            pair_copy(c).start()

        each(per_piece, one_chunk)

    def join(u):
        def one_chunk(i):
            c = u * per_piece + i
            pair_copy(c).wait_recv()
            span = pl.ds(c * chunk, chunk)
            w_out[:, span] = z_out[my_kind, :, span] + p_in[:, span]
            for k in range(1, pairs):
                z_copy(c, k).start()

        each(per_piece, one_chunk)

    def collect(u):
        def one_chunk(i):
            c = u * per_piece + i
            span = pl.ds(c * chunk, chunk)
            total = 0.5 * core[span] + w_out[my_pair, span]
            for k in range(1, pairs):
                z_copy(c, k).wait_recv()
                total += w_in[k - 1, span]
            j, s = lax.div(c, steps), lax.rem(c, steps)
            own[j, pl.ds(s * chunk, chunk)] = total

            @pl.when(j != me)
            def _():
                y_forward(0, s, lax.rem(j - me + bands, bands)).start()

            @pl.when(j == me)
            def _():
                gy[0, pl.ds(s * chunk, chunk), my_block] = total

        each(per_piece, one_chunk)
        group = piece_rows // r_part
        rows_here = own[pl.ds(u * group, group)].reshape(piece_rows, block, z_cells)
        start = pl.multiple_of(u * piece_rows, TILE)
        there = pl.multiple_of(slab * rows + u * piece_rows, TILE)
        line[0, :, pl.ds(start, piece_rows)] = turned(rows_here)
        for k in range(1, grids):
            x_piece(u, k).start()
        gx[0, :, pl.ds(there, piece_rows)] = line[
            0, pl.ds(slab * y_part, y_part), pl.ds(start, piece_rows)
        ]

    squares(0)
    squares(1)
    pl.semaphore_wait(barrier, len(partners))
    send_squares(0)
    send_squares(1)
    core_copy().wait()

    def sum_step(u):
        forward(u)

        @pl.when(u + 2 < pieces)
        def _():
            squares(u + 2)
            send_squares(u + 2)

        @pl.when(u >= 1)
        def _():
            join(u - 1)

        @pl.when(u >= 2)
        def _():
            collect(u - 2)

    each(pieces, sum_step)
    join(pieces - 1)
    collect(pieces - 2)
    collect(pieces - 1)

    swap_in(0).start()
    dz[...] = along_third(own[...])
    swap_in(1).start()
    along_second(0, 0)
    for u in range(pieces):
        for k in range(1, grids):
            x_piece(u, k).wait_recv()
    along_first(0)
    for s in range(1, steps):
        along_second(0, s)
    dx[...] = end_first(0)
    swap_in(2).start()
    for f in range(3):
        swap_in(f).wait()

    def potential_rows(j, row):
        span = pl.ds(row, xc_rows)
        here = (spin * half + j, span)
        there = (j, span)
        n_own, n_other = own[here], other[(0,) + there]
        g_own = [dx[here], sy[(0,) + here], dz[here]]
        g_other = [other[(2,) + there], other[(3,) + there], other[(1,) + there]]
        s_own = g_own[0] * g_own[0] + g_own[1] * g_own[1] + g_own[2] * g_own[2]
        s_mix = g_own[0] * g_other[0] + g_own[1] * g_other[1] + g_own[2] * g_other[2]
        s_other = g_other[0] * g_other[0] + g_other[1] * g_other[1] + g_other[2] * g_other[2]
        energy, pull = jax.vjp(xc_energy, n_own, n_other, s_own, s_mix, s_other)
        derivs = pull(jnp.ones_like(energy))
        fields[(0,) + here] = derivs[0]
        outgoing[(0,) + there] = derivs[1]
        for a in range(3):
            fields[(1 + a,) + here] = 2.0 * derivs[2] * g_own[a] + derivs[3] * g_other[a]
            outgoing[(1 + a,) + there] = 2.0 * derivs[4] * g_other[a] + derivs[3] * g_own[a]

    def flux_out(s):
        swap_out(s).wait_recv()
        for k in range(1, bands):
            y_forward(1, s, k).start()
        span = pl.ds(s * chunk, chunk)
        gy[1, span, my_block] = fields[2, me, span]

    end_second(0, 0)
    swap_steep(0).start()
    for s in range(steps):
        swap_steep(s).wait_recv()
        per_group = chunk // xc_rows
        each(
            half * per_group,
            lambda i: potential_rows(
                lax.div(i, per_group), s * chunk + lax.rem(i, per_group) * xc_rows
            ),
        )
        swap_out(s).start()
        if s + 1 < steps:
            end_second(0, s + 1)
            swap_steep(s + 1).start()
        flux_out(s)

    line[1] = turned(whole(fields[1]))
    for k in range(1, grids):
        x_whole(k).start()
    gx[1, :, my_slab] = line[1, pl.ds(slab * y_part, y_part)]
    for s in range(steps - 1):
        along_second(1, s)
    dz[...] = fields[0] - along_third(fields[3])
    for k in range(1, grids):
        x_whole(k).wait_recv()
    along_first(1)
    along_second(1, steps - 1)
    dz[...] = dz[...] - end_first(1)
    for s in range(steps):
        end_second(1, s)
    out_ref[...] = whole(dz[...] - sy[1])

    def drain(c):
        x_copy(c).wait_send()
        pair_copy(c).wait_send()
        for k in range(1, pairs):
            z_copy(c, k).wait_send()

    each(chunks, drain)
    for k in range(1, grids):
        for u in range(pieces):
            x_piece(u, k).wait_send()
        x_whole(k).wait_send()
        x_back(0, k).wait_send()
        x_back(1, k).wait_send()
    for t in range(2):
        for s in range(steps):
            for k in range(1, bands):
                y_forward(t, s, k).wait_send()
                y_back(t, s, k).wait_send()
    for s in range(steps):
        swap_steep(s).wait_send()
        swap_out(s).wait_send()


def potential_call(orbitals, partial_bands, core_density, tables):
    bands, grids = lax.axis_size("band"), lax.axis_size("grid")
    _, count, rows, y_cells, z_cells = orbitals.shape
    block, slow = y_cells // bands, bands // FAST
    y_part, r_part = block // grids, rows // bands
    x_cells = rows * grids
    steps = r_part // math.gcd(CHUNK, r_part)
    chunks = bands * steps
    pieces = rows // max(r_part, TILE)
    half = bands // 2
    vmem = pl.BlockSpec(memory_space=pltpu.VMEM)
    hbm = pl.BlockSpec(memory_space=pl.ANY)
    dma = pltpu.SemaphoreType.DMA
    real = jnp.float32
    cells = (bands, r_part, block, z_cells)
    return pl.pallas_call(
        functools.partial(potential_kernel, bands, grids),
        out_shape=jax.ShapeDtypeStruct((rows, block, z_cells), real),
        in_specs=[pl.BlockSpec(memory_space=pltpu.SMEM), hbm, hbm] + [vmem] * 3,
        out_specs=vmem,
        scratch_shapes=[
            pltpu.VMEM((count, rows, y_cells, z_cells), jnp.bfloat16),
            pltpu.VMEM((rows, block, z_cells), real),
            pltpu.VMEM((FAST, rows, slow, block, z_cells), real),
            pltpu.VMEM((rows, slow, block, z_cells), real),
            pltpu.VMEM((2, slow // 2, rows, block, z_cells), real),
            pltpu.VMEM((slow // 2, rows, block, z_cells), real),
            pltpu.VMEM((slow // 2, rows, block, z_cells), real),
            pltpu.VMEM((slow // 2 - 1, rows, block, z_cells), real),
            pltpu.VMEM(cells, real),
            pltpu.VMEM((2, block, rows, z_cells), real),
            pltpu.VMEM((2, y_part, x_cells, z_cells), real),
            pltpu.VMEM((2, y_part, x_cells, z_cells), real),
            pltpu.VMEM((2, block, rows, z_cells), real),
            pltpu.VMEM((2, r_part, y_cells, z_cells), real),
            pltpu.VMEM((2, r_part, y_cells, z_cells), real),
            pltpu.VMEM((2,) + cells, real),
            pltpu.VMEM(cells, real),
            pltpu.VMEM(cells, real),
            pltpu.VMEM((4, half) + cells[1:], real),
            pltpu.VMEM((4,) + cells, real),
            pltpu.VMEM((4, half) + cells[1:], real),
            dma((pieces,)),
            dma,
            dma((chunks,)),
            dma((chunks,)),
            dma((chunks,)),
            dma((chunks,)),
            dma((slow // 2 - 1, chunks)),
            dma((slow // 2 - 1, chunks)),
        ]
        + [dma((pieces, grids - 1))] * 2
        + [dma((grids - 1,))] * 2
        + [dma((2, grids - 1))] * 2
        + [dma((2, steps, bands - 1))] * 4
        + [dma((3,))] * 2
        + [dma((steps,))] * 4,
        compiler_params=pltpu.CompilerParams(
            collective_id=0, has_side_effects=True, vmem_limit_bytes=60 * 2**20
        ),
        name="potential",
    )(partial_bands, orbitals, core_density, *tables)


def per_device(orbitals, partial_bands, core_density):
    x_rows, y_cols, z_cells = core_density.shape
    tables = (
        jnp.asarray(spectral_table(x_rows * lax.axis_size("grid"))),
        jnp.asarray(spectral_table(y_cols)),
        jnp.asarray(spectral_table(z_cells).T),
    )
    return potential_call(orbitals, partial_bands, core_density, tables)[None]


def solution(mesh):
    in_specs = (P("spin", "band", "grid", None, None), P("spin", None), P("grid", None, None))
    out_specs = P("spin", "grid", "band", None)
    return jax.shard_map(
        per_device, mesh=mesh, in_specs=in_specs, out_specs=out_specs, check_vma=False
    )
```

```python
import functools
import math

import jax
import jax.numpy as jnp
import numpy as np
from jax import lax
from jax.experimental import pallas as pl
from jax.experimental.pallas import tpu as pltpu
from jax.sharding import PartitionSpec as P

KAPPA = 0.804
MU_X = 0.2195149727645171
BETA = 0.06672455060314922
GAMMA = (1.0 - math.log(2.0)) / math.pi**2
FZ_NORM = 2.0 ** (4.0 / 3.0) - 2.0
FPP_ZERO = 1.709921
EXACT = lax.Precision.HIGHEST
MESH = pl.DeviceIdType.MESH
CHUNK = 4
FAST = 2
XC_ROWS = 2
TILE = 8


def cube_root(value):
    return jnp.exp(jnp.log(value) * (1.0 / 3.0))


def pw_fit(radius, root, amp, alpha, beta_one, beta_two, beta_three, beta_four):
    denom = (2.0 * amp) * (
        root * (beta_one + root * (beta_two + root * (beta_three + root * beta_four)))
    )
    return -2.0 * amp * (1.0 + alpha * radius) * jnp.log(1.0 + 1.0 / denom)


def exchange_part(double, sigma_four):
    kfermi = (3.0 * math.pi**2) ** (1.0 / 3.0) * cube_root(double)
    product = kfermi * double
    scaled = sigma_four / (4.0 * product * product)
    enhance = 1.0 + KAPPA - KAPPA / (1.0 + MU_X * scaled / KAPPA)
    return -0.75 / math.pi * product * enhance


def xc_energy(n_up, n_down, s_uu, s_ud, s_dd):
    exch = 0.5 * (exchange_part(2.0 * n_up, 4.0 * s_uu) + exchange_part(2.0 * n_down, 4.0 * s_dd))
    total = n_up + n_down
    zeta = (n_up - n_down) / total
    third = cube_root(total)
    radius = (3.0 / (4.0 * math.pi)) ** (1.0 / 3.0) / third
    root = jnp.sqrt(radius)
    ec_para = pw_fit(radius, root, 0.031091, 0.2137, 7.5957, 3.5876, 1.6382, 0.49294)
    ec_ferro = pw_fit(radius, root, 0.015545, 0.20548, 14.1189, 6.1977, 3.3662, 0.62517)
    neg_stiff = pw_fit(radius, root, 0.016887, 0.11125, 10.357, 3.6231, 0.88026, 0.49671)
    plus_z = 1.0 + zeta
    minus_z = 1.0 - zeta
    plus_third = cube_root(plus_z)
    minus_third = cube_root(minus_z)
    fzeta = (plus_z * plus_third + minus_z * minus_third - 2.0) * (1.0 / FZ_NORM)
    zeta_sq = zeta * zeta
    zeta_four = zeta_sq * zeta_sq
    ec_lda = (
        ec_para
        - neg_stiff * fzeta * (1.0 / FPP_ZERO) * (1.0 - zeta_four)
        + (ec_ferro - ec_para) * fzeta * zeta_four
    )
    phi = 0.5 * (plus_third * plus_third + minus_third * minus_third)
    phi_cube = phi * phi * phi
    kfermi = (3.0 * math.pi**2) ** (1.0 / 3.0) * third
    screen_sq = kfermi * (4.0 / math.pi)
    sigma = s_uu + 2.0 * s_ud + s_dd
    tsq = sigma / (4.0 * phi * phi * screen_sq * total * total)
    amp = BETA / GAMMA / (jnp.exp(-ec_lda / (GAMMA * phi_cube)) - 1.0)
    atsq = amp * tsq
    gradient_term = (
        GAMMA
        * phi_cube
        * jnp.log(1.0 + BETA / GAMMA * tsq * (1.0 + atsq) / (1.0 + atsq + atsq * atsq))
    )
    return exch + total * (ec_lda + gradient_term)


def spectral_table(length):
    index = np.arange(length)
    angle = 2.0 * np.pi / length * (index[:, None] * index[None, :] % length)
    mode = np.where(index < length // 2, index, index - length)
    mode = np.where(index == length // 2, 0, mode)
    wave = 2.0 * np.pi / length * mode
    sines, cosines = np.sin(angle), np.cos(angle)
    first_term = (sines * wave[None, :]) @ cosines.T
    second_term = (cosines * wave[None, :]) @ sines.T
    return ((second_term - first_term) / length).astype(np.float32)


def potential_kernel(
    bands,
    grids,
    pairs_ref,
    orb_hbm,
    core_hbm,
    tx_ref,
    ty_ref,
    tz_ref,
    out_ref,
    orb,
    core,
    part,
    x_in,
    z_out,
    p_in,
    w_out,
    w_in,
    own,
    line,
    gx,
    hx,
    sx,
    gy,
    hy,
    sy,
    dx,
    dz,
    other,
    fields,
    outgoing,
    orb_sem,
    core_sem,
    x_send,
    x_recv,
    p_send,
    p_recv,
    w_send,
    w_recv,
    xp_send,
    xp_recv,
    xf_send,
    xf_recv,
    xb_send,
    xb_recv,
    yf_send,
    yf_recv,
    yb_send,
    yb_recv,
    in_send,
    in_recv,
    gy_send,
    gy_recv,
    out_send,
    out_recv,
):
    count, rows, y_cells, z_cells = orb.shape
    block = core.shape[1]
    slow = bands // FAST
    steps = out_send.shape[0]
    r_part = rows // bands
    chunk = r_part // steps
    piece_rows = rows // xp_send.shape[0]
    pieces = rows // piece_rows
    per_piece = piece_rows // chunk
    chunks = rows // chunk
    y_part = block // grids
    half = bands // 2
    xc_rows = math.gcd(XC_ROWS, chunk)
    me = lax.axis_index("band")
    slab = lax.axis_index("grid")
    spin = lax.axis_index("spin")
    my_slow, my_fast = lax.div(me, FAST), lax.rem(me, FAST)
    partner = {"band": my_slow * FAST + (1 - my_fast)}
    pairs = slow // 2
    my_pair = lax.div(my_slow, 2)
    my_kind = lax.rem(my_slow + my_pair, 2)
    beside = {"band": (my_slow + 1 - 2 * lax.rem(my_slow, 2)) * FAST + my_fast}
    twin = {"spin": 1 - spin}
    my_block = pl.ds(pl.multiple_of(me * block, TILE), block)
    my_slab = pl.ds(pl.multiple_of(slab * rows, TILE), rows)
    mine = pl.ds(spin * half, half)
    theirs = pl.ds((1 - spin) * half, half)

    def remote(src, dst, send, recv, device):
        return pltpu.make_async_remote_copy(
            src_ref=src,
            dst_ref=dst,
            send_sem=send,
            recv_sem=recv,
            device_id=device,
            device_id_type=MESH,
        )

    def orb_copy(u):
        span = pl.ds(u * piece_rows, piece_rows)
        return pltpu.make_async_copy(orb_hbm.at[0, :, span], orb.at[:, span], orb_sem.at[u])

    def core_copy():
        return pltpu.make_async_copy(core_hbm.at[:, my_block], core, core_sem)

    def x_copy(c):
        span = pl.ds(c * chunk, chunk)
        return remote(
            part.at[1 - my_fast, span], x_in.at[span], x_send.at[c], x_recv.at[c], partner
        )

    def pair_copy(c):
        span = pl.ds(c * chunk, chunk)
        return remote(
            z_out.at[1 - my_kind, :, span],
            p_in.at[:, span],
            p_send.at[c],
            p_recv.at[c],
            beside,
        )

    def z_copy(c, k):
        span = pl.ds(c * chunk, chunk)
        h = lax.rem(my_pair + k, pairs)
        return remote(
            w_out.at[h, span],
            w_in.at[k - 1, span],
            w_send.at[k - 1, c],
            w_recv.at[k - 1, c],
            {"band": (2 * h + lax.rem(my_kind + h, 2)) * FAST + my_fast},
        )

    def x_piece(u, k):
        q = lax.rem(slab + k, grids)
        start = pl.multiple_of(u * piece_rows, TILE)
        there = pl.multiple_of(slab * rows + u * piece_rows, TILE)
        return remote(
            line.at[0, pl.ds(q * y_part, y_part), pl.ds(start, piece_rows)],
            gx.at[0, :, pl.ds(there, piece_rows)],
            xp_send.at[u, k - 1],
            xp_recv.at[u, k - 1],
            {"grid": q},
        )

    def x_whole(k):
        q = lax.rem(slab + k, grids)
        return remote(
            line.at[1, pl.ds(q * y_part, y_part)],
            gx.at[1, :, my_slab],
            xf_send.at[k - 1],
            xf_recv.at[k - 1],
            {"grid": q},
        )

    def x_back(t, k):
        q = lax.rem(slab + k, grids)
        return remote(
            hx.at[t, :, pl.ds(pl.multiple_of(q * rows, TILE), rows)],
            sx.at[t, pl.ds(slab * y_part, y_part)],
            xb_send.at[t, k - 1],
            xb_recv.at[t, k - 1],
            {"grid": q},
        )

    def y_forward(t, s, k):
        q = lax.rem(me + k, bands)
        source = own if t == 0 else fields.at[2]
        return remote(
            source.at[q, pl.ds(s * chunk, chunk)],
            gy.at[t, pl.ds(s * chunk, chunk), my_block],
            yf_send.at[t, s, k - 1],
            yf_recv.at[t, s, k - 1],
            {"band": q},
        )

    def y_back(t, s, k):
        q = lax.rem(me + k, bands)
        return remote(
            hy.at[t, pl.ds(s * chunk, chunk), pl.ds(pl.multiple_of(q * block, TILE), block)],
            sy.at[t, me, pl.ds(s * chunk, chunk)],
            yb_send.at[t, s, k - 1],
            yb_recv.at[t, s, k - 1],
            {"band": q},
        )

    incoming = [own, dz, dx]

    def swap_in(f):
        return remote(incoming[f].at[theirs], other.at[f], in_send.at[f], in_recv.at[f], twin)

    def swap_steep(s):
        span = pl.ds(s * chunk, chunk)
        return remote(
            sy.at[0, theirs, span], other.at[3, :, span], gy_send.at[s], gy_recv.at[s], twin
        )

    def swap_out(s):
        span = pl.ds(s * chunk, chunk)
        return remote(
            outgoing.at[:, :, span],
            fields.at[:, mine, span],
            out_send.at[s],
            out_recv.at[s],
            twin,
        )

    def times(table, field):
        return jnp.dot(table, field, precision=EXACT, preferred_element_type=jnp.float32)

    def turned(value):
        return jnp.transpose(value, (1, 0, 2))

    def whole(value):
        return value.reshape(rows, block, z_cells)

    def split(value):
        return value.reshape(bands, r_part, block, z_cells)

    def along_third(field):
        return times(field.reshape(rows * block, z_cells), tz_ref[...]).reshape(field.shape)

    def along_first(t):
        for y in range(y_part):
            hx[t, y] = times(tx_ref[...], gx[t, y])
        for k in range(1, grids):
            x_back(t, k).start()
        sx[t, pl.ds(slab * y_part, y_part)] = hx[t, :, my_slab]

    def along_second(t, s):
        for k in range(1, bands):
            y_forward(t, s, k).wait_recv()
        for r in range(s * chunk, (s + 1) * chunk):
            hy[t, r] = times(ty_ref[...], gy[t, r])
        for k in range(1, bands):
            y_back(t, s, k).start()
        span = pl.ds(s * chunk, chunk)
        sy[t, me, span] = hy[t, span, my_block]

    def end_first(t):
        for k in range(1, grids):
            x_back(t, k).wait_recv()
        return split(turned(sx[t]))

    def end_second(t, s):
        for k in range(1, bands):
            y_back(t, s, k).wait_recv()

    def each(number, body):
        lax.fori_loop(0, number, lambda i, carry: (body(i), carry)[1], 0)

    def order(u):
        if pieces != bands:
            return u
        v, fast = u % slow, u // slow
        late = v // pairs
        return (v + late * (pairs + slow - 1 - 2 * v)) * FAST + fast

    each(pieces, lambda u: orb_copy(order(u)).start())
    core_copy().start()
    partners = (
        [twin]
        + [{"grid": lax.rem(slab + k, grids)} for k in range(1, grids)]
        + [{"band": lax.rem(me + k, bands)} for k in range(1, bands)]
    )
    barrier = pltpu.get_barrier_semaphore()
    for target in partners:
        pl.semaphore_signal(barrier, inc=1, device_id=target, device_id_type=MESH)
    first = pairs_ref[0, 0]
    last = first + pairs_ref[0, 1]
    weights = []
    for n in range(count):
        ident = me * count + n
        weights.append(jnp.where((ident >= first) & (ident < last), 0.5, 1.0).astype(jnp.float32))

    def squares(u):
        orb_copy(u).wait()

        def one_chunk(i):
            c = u * per_piece + i
            for r in range(chunk):
                row = c * chunk + r
                for b in range(bands):
                    total = jnp.zeros((block, z_cells), jnp.float32)
                    for n in range(count):
                        values = orb[n, row, b * block : (b + 1) * block].astype(jnp.float32)
                        total += weights[n] * (values * values)
                    part[b % FAST, row, b // FAST] = total

        each(per_piece, one_chunk)

    def send_squares(u):
        each(per_piece, lambda i: x_copy(u * per_piece + i).start())

    def forward(u):
        def one_chunk(i):
            c = u * per_piece + i
            x_copy(c).wait_recv()
            span = pl.ds(c * chunk, chunk)
            for d in range(slow):
                z_out[(d + d // 2) % 2, d // 2, span] = part[my_fast, span, d] + x_in[span, d]
            pair_copy(c).start()

        each(per_piece, one_chunk)

    def join(u):
        def one_chunk(i):
            c = u * per_piece + i
            pair_copy(c).wait_recv()
            span = pl.ds(c * chunk, chunk)
            w_out[:, span] = z_out[my_kind, :, span] + p_in[:, span]
            for k in range(1, pairs):
                z_copy(c, k).start()

        each(per_piece, one_chunk)

    def collect(u):
        def one_chunk(i):
            c = u * per_piece + i
            span = pl.ds(c * chunk, chunk)
            total = 0.5 * core[span] + w_out[my_pair, span]
            for k in range(1, pairs):
                z_copy(c, k).wait_recv()
                total += w_in[k - 1, span]
            j, s = lax.div(c, steps), lax.rem(c, steps)
            own[j, pl.ds(s * chunk, chunk)] = total

            @pl.when(j != me)
            def _():
                y_forward(0, s, lax.rem(j - me + bands, bands)).start()

            @pl.when(j == me)
            def _():
                gy[0, pl.ds(s * chunk, chunk), my_block] = total

        each(per_piece, one_chunk)
        group = piece_rows // r_part
        rows_here = own[pl.ds(u * group, group)].reshape(piece_rows, block, z_cells)
        start = pl.multiple_of(u * piece_rows, TILE)
        there = pl.multiple_of(slab * rows + u * piece_rows, TILE)
        line[0, :, pl.ds(start, piece_rows)] = turned(rows_here)
        for k in range(1, grids):
            x_piece(u, k).start()
        gx[0, :, pl.ds(there, piece_rows)] = line[
            0, pl.ds(slab * y_part, y_part), pl.ds(start, piece_rows)
        ]

    squares(order(0))
    squares(order(1))
    pl.semaphore_wait(barrier, len(partners))
    send_squares(order(0))
    send_squares(order(1))
    core_copy().wait()

    def sum_step(u):
        forward(order(u))

        @pl.when(u + 2 < pieces)
        def _():
            squares(order(u + 2))
            send_squares(order(u + 2))

        @pl.when(u >= 1)
        def _():
            join(order(u - 1))

        @pl.when(u >= 2)
        def _():
            collect(order(u - 2))

    each(pieces, sum_step)
    join(order(pieces - 1))
    collect(order(pieces - 2))
    collect(order(pieces - 1))

    swap_in(0).start()
    dz[...] = along_third(own[...])
    swap_in(1).start()
    along_second(0, 0)
    for u in range(pieces):
        for k in range(1, grids):
            x_piece(u, k).wait_recv()
    along_first(0)
    for s in range(1, steps):
        along_second(0, s)
    dx[...] = end_first(0)
    swap_in(2).start()
    for f in range(3):
        swap_in(f).wait()

    def potential_rows(j, row):
        span = pl.ds(row, xc_rows)
        here = (spin * half + j, span)
        there = (j, span)
        n_own, n_other = own[here], other[(0,) + there]
        g_own = [dx[here], sy[(0,) + here], dz[here]]
        g_other = [other[(2,) + there], other[(3,) + there], other[(1,) + there]]
        s_own = g_own[0] * g_own[0] + g_own[1] * g_own[1] + g_own[2] * g_own[2]
        s_mix = g_own[0] * g_other[0] + g_own[1] * g_other[1] + g_own[2] * g_other[2]
        s_other = g_other[0] * g_other[0] + g_other[1] * g_other[1] + g_other[2] * g_other[2]
        energy, pull = jax.vjp(xc_energy, n_own, n_other, s_own, s_mix, s_other)
        derivs = pull(jnp.ones_like(energy))
        fields[(0,) + here] = derivs[0]
        outgoing[(0,) + there] = derivs[1]
        for a in range(3):
            fields[(1 + a,) + here] = 2.0 * derivs[2] * g_own[a] + derivs[3] * g_other[a]
            outgoing[(1 + a,) + there] = 2.0 * derivs[4] * g_other[a] + derivs[3] * g_own[a]

    def flux_out(s):
        swap_out(s).wait_recv()
        for k in range(1, bands):
            y_forward(1, s, k).start()
        span = pl.ds(s * chunk, chunk)
        gy[1, span, my_block] = fields[2, me, span]

    end_second(0, 0)
    swap_steep(0).start()
    for s in range(steps):
        swap_steep(s).wait_recv()
        per_group = chunk // xc_rows
        each(
            half * per_group,
            lambda i: potential_rows(
                lax.div(i, per_group), s * chunk + lax.rem(i, per_group) * xc_rows
            ),
        )
        swap_out(s).start()
        if s + 1 < steps:
            end_second(0, s + 1)
            swap_steep(s + 1).start()
        flux_out(s)

    line[1] = turned(whole(fields[1]))
    for k in range(1, grids):
        x_whole(k).start()
    gx[1, :, my_slab] = line[1, pl.ds(slab * y_part, y_part)]
    for s in range(steps - 1):
        along_second(1, s)
    dz[...] = fields[0] - along_third(fields[3])
    for k in range(1, grids):
        x_whole(k).wait_recv()
    along_first(1)
    along_second(1, steps - 1)
    dz[...] = dz[...] - end_first(1)
    for s in range(steps):
        end_second(1, s)
    out_ref[...] = whole(dz[...] - sy[1])

    def drain(c):
        x_copy(c).wait_send()
        pair_copy(c).wait_send()
        for k in range(1, pairs):
            z_copy(c, k).wait_send()

    each(chunks, drain)
    for k in range(1, grids):
        for u in range(pieces):
            x_piece(u, k).wait_send()
        x_whole(k).wait_send()
        x_back(0, k).wait_send()
        x_back(1, k).wait_send()
    for t in range(2):
        for s in range(steps):
            for k in range(1, bands):
                y_forward(t, s, k).wait_send()
                y_back(t, s, k).wait_send()
    for s in range(steps):
        swap_steep(s).wait_send()
        swap_out(s).wait_send()


def potential_call(orbitals, partial_bands, core_density, tables):
    bands, grids = lax.axis_size("band"), lax.axis_size("grid")
    _, count, rows, y_cells, z_cells = orbitals.shape
    block, slow = y_cells // bands, bands // FAST
    y_part, r_part = block // grids, rows // bands
    x_cells = rows * grids
    steps = r_part // math.gcd(CHUNK, r_part)
    chunks = bands * steps
    pieces = rows // max(r_part, TILE)
    half = bands // 2
    vmem = pl.BlockSpec(memory_space=pltpu.VMEM)
    hbm = pl.BlockSpec(memory_space=pl.ANY)
    dma = pltpu.SemaphoreType.DMA
    real = jnp.float32
    cells = (bands, r_part, block, z_cells)
    return pl.pallas_call(
        functools.partial(potential_kernel, bands, grids),
        out_shape=jax.ShapeDtypeStruct((rows, block, z_cells), real),
        in_specs=[pl.BlockSpec(memory_space=pltpu.SMEM), hbm, hbm] + [vmem] * 3,
        out_specs=vmem,
        scratch_shapes=[
            pltpu.VMEM((count, rows, y_cells, z_cells), jnp.bfloat16),
            pltpu.VMEM((rows, block, z_cells), real),
            pltpu.VMEM((FAST, rows, slow, block, z_cells), real),
            pltpu.VMEM((rows, slow, block, z_cells), real),
            pltpu.VMEM((2, slow // 2, rows, block, z_cells), real),
            pltpu.VMEM((slow // 2, rows, block, z_cells), real),
            pltpu.VMEM((slow // 2, rows, block, z_cells), real),
            pltpu.VMEM((slow // 2 - 1, rows, block, z_cells), real),
            pltpu.VMEM(cells, real),
            pltpu.VMEM((2, block, rows, z_cells), real),
            pltpu.VMEM((2, y_part, x_cells, z_cells), real),
            pltpu.VMEM((2, y_part, x_cells, z_cells), real),
            pltpu.VMEM((2, block, rows, z_cells), real),
            pltpu.VMEM((2, r_part, y_cells, z_cells), real),
            pltpu.VMEM((2, r_part, y_cells, z_cells), real),
            pltpu.VMEM((2,) + cells, real),
            pltpu.VMEM(cells, real),
            pltpu.VMEM(cells, real),
            pltpu.VMEM((4, half) + cells[1:], real),
            pltpu.VMEM((4,) + cells, real),
            pltpu.VMEM((4, half) + cells[1:], real),
            dma((pieces,)),
            dma,
            dma((chunks,)),
            dma((chunks,)),
            dma((chunks,)),
            dma((chunks,)),
            dma((slow // 2 - 1, chunks)),
            dma((slow // 2 - 1, chunks)),
        ]
        + [dma((pieces, grids - 1))] * 2
        + [dma((grids - 1,))] * 2
        + [dma((2, grids - 1))] * 2
        + [dma((2, steps, bands - 1))] * 4
        + [dma((3,))] * 2
        + [dma((steps,))] * 4,
        compiler_params=pltpu.CompilerParams(
            collective_id=0, has_side_effects=True, vmem_limit_bytes=60 * 2**20
        ),
        name="potential",
    )(partial_bands, orbitals, core_density, *tables)


def per_device(orbitals, partial_bands, core_density):
    x_rows, y_cols, z_cells = core_density.shape
    tables = (
        jnp.asarray(spectral_table(x_rows * lax.axis_size("grid"))),
        jnp.asarray(spectral_table(y_cols)),
        jnp.asarray(spectral_table(z_cells).T),
    )
    return potential_call(orbitals, partial_bands, core_density, tables)[None]


def solution(mesh):
    in_specs = (P("spin", "band", "grid", None, None), P("spin", None), P("grid", None, None))
    out_specs = P("spin", "grid", "band", None)
    return jax.shard_map(
        per_device, mesh=mesh, in_specs=in_specs, out_specs=out_specs, check_vma=False
    )
```
